32 devices in a mesh: section: 4 (over z), tensor: 4 (over y, x), dp: 2 (over core).
Axes of the slice: x: 2, y: 2, z: 4, core: 2. Of those that a mesh axis runs over, the one named last changes fastest.
Arguments:
- forward_rows: bfloat16 [4, 2, 192, 8192], P('section', 'dp', None, 'tensor'), may hold values from -6 to 6
- saved_rows: bfloat16 [4, 2, 192, 8192], P('section', 'dp', None, 'tensor'), may hold values from -40.5 to 40.5
- output_grad: bfloat16 [4, 2, 192, 8192], P('section', 'dp', None, 'tensor'), may hold values from -1.27 to 1.27
- lengths: int32 [4, 2, 2], P('section', 'dp'), may hold values from 1 to 96
- norm_gain: bfloat16 [4, 8192], P('section', 'tensor'), may hold values from 0.5 to 1.5
- down_map: bfloat16 [4, 192, 8192], P('section', None, 'tensor'), may hold values from -0.067396115 to 0.067396115
- up_map: bfloat16 [4, 192, 8192], P('section', None, 'tensor'), may hold values from -1.0625 to 1.0625
Outputs:
- next_inputs: bfloat16 [4, 2, 192, 8192], P('section', 'dp', None, 'tensor')
- next_grads: bfloat16 [4, 2, 192, 8192], P('section', 'dp', None, 'tensor')
- grad_down: bfloat16 [4, 192, 8192], P('section', 'dp', 'tensor')
- grad_up: bfloat16 [4, 192, 8192], P('section', 'dp', 'tensor')
The draws below stay inside these ranges and needn't reach their ends.
All inputs are finite; a program needn't handle non-finite values.
Results may differ from the reference program's by a relative error of at most 0.02.
Values may be sent and summed in bfloat16 or wider, within the bound.
A program may use at most 64 MiB of HBM per device.

```python
import jax
import jax.numpy as jnp
from jax import lax

D = 8192
R = 192
ROWS = 192
SEQ = 96
N_SECTION = 4
N_DP = 2


def shared_rows(key):
    base = jax.random.fold_in(key, 11)
    shape = (N_SECTION, N_DP, ROWS, D)
    return jnp.clip(jax.random.normal(base, shape, jnp.float32), -6.0, 6.0)


def draw_saved_rows(key, part):
    values = shared_rows(key)
    return values.astype(jnp.bfloat16)


def draw_output_grad(key, part):
    shared = shared_rows(key)
    noise = jax.random.normal(jax.random.fold_in(key, 13), shared.shape, jnp.float32)
    mixed = 0.8 * shared + 0.6 * jnp.clip(noise, -6.0, 6.0)
    return (0.15 * mixed).astype(jnp.bfloat16)


def map_values(key, salt):
    base = jax.random.fold_in(key, salt)
    shape = (N_SECTION, R, D)
    return jnp.clip(jax.random.normal(base, shape, jnp.float32), -6.0, 6.0)


def draw_down_map(key, part):
    return (map_values(key, 21) * D ** (-0.5)).astype(jnp.bfloat16)


def draw_up_map(key, part):
    shared = map_values(key, 21)
    own_part = map_values(key, 22)
    mixed = 0.8 * shared + 0.6 * own_part
    return (mixed * (R // 3) ** (-0.5)).astype(jnp.bfloat16)


def place_ends(result, key, smallest, top_value):
    extent = result.shape
    place = [jax.random.randint(jax.random.fold_in(key, axis), (), 0, extent[axis]) for axis in range(len(extent))]
    result = result.at[tuple(place)].set(smallest)
    longest = extent.index(max(extent))
    place[longest] = (place[longest] + 1) % extent[longest]
    return result.at[tuple(place)].set(top_value)


def level_of(rng, extent, split, smallest, high):
    gain, own = 1.0, jax.random.fold_in(rng, 6)
    for dim, parts in split:
        draws = jnp.exp(jax.random.uniform(jax.random.fold_in(own, dim), (parts,), jnp.float32, smallest / len(split), high / len(split)))
        gain = gain * jnp.repeat(draws, extent[dim] // parts).reshape([-1 if axis == dim else 1 for axis in range(len(extent))])
    return gain


def normal_values(stream_key, dims, scale, most, pieces=(), held_as=jnp.bfloat16):
    factor_of = level_of(stream_key, dims, pieces, -0.22, 0.18) if pieces else 1.0
    values = jax.random.normal(stream_key, dims, jnp.float32) * scale * factor_of
    return jnp.minimum(jnp.maximum(values, -most), most).astype(held_as)


def setup_inputs(seed: int = 0) -> dict:
    seeds = jax.random.split(jax.random.key(seed), 8)
    forward_rows = normal_values(seeds[0], (N_SECTION, N_DP, ROWS, D), 1.0, 6.0, ((0, 4), (1, 2), (3, 4)))
    saved_rows = draw_saved_rows(jax.random.fold_in(seeds[7], 71), 0)
    output_grad = draw_output_grad(jax.random.fold_in(seeds[7], 71), 0)
    lengths = place_ends(jax.random.randint(seeds[3], (N_SECTION, N_DP, 2), 1, SEQ + 1), jax.random.fold_in(seeds[3], 1), 1, SEQ).astype(jnp.int32)
    norm_gain = jnp.clip(1.0 + 0.1 * jax.random.normal(seeds[4], (N_SECTION, D), jnp.float32), 0.5, 1.5).astype(jnp.bfloat16)
    down_map = draw_down_map(jax.random.fold_in(seeds[7], 71), 0)
    up_map = draw_up_map(jax.random.fold_in(seeds[7], 71), 0)
    return dict(forward_rows=forward_rows, saved_rows=saved_rows, output_grad=output_grad, lengths=lengths, norm_gain=norm_gain, down_map=down_map, up_map=up_map)


EPSILON = 1e-05

def contract_last(left_side, right_side):
    return lax.dot_general(left_side, right_side, (((1,), (1,)), ((), ())), preferred_element_type=jnp.float32)

def contract_rows(left_side, right_side):
    return lax.dot_general(left_side, right_side, (((0,), (0,)), ((), ())), preferred_element_type=jnp.float32)

def silu_slope(values):
    gate_value = jax.nn.sigmoid(values)
    return gate_value * (1.0 + values * (1.0 - gate_value))

def norm_rows(row_block, gain_cols):
    values = row_block.astype(jnp.float32)
    scale = lax.rsqrt(lax.optimization_barrier(jnp.mean(values * values, axis=1, keepdims=True)) + EPSILON)
    return (values, scale, (values * scale * gain_cols).astype(jnp.bfloat16))

def group_tick(forward_block, saved_block, incoming, seq_lengths, gain_cols, down_rows, up_rows):
    forward_values, forward_scale, forward_normed = norm_rows(forward_block, gain_cols)
    forward_act = jax.nn.silu(contract_last(forward_normed, down_rows)).astype(jnp.bfloat16)
    forward_out = (forward_values + jnp.dot(forward_act, up_rows, preferred_element_type=jnp.float32)).astype(jnp.bfloat16)
    position = jnp.arange(ROWS, dtype=jnp.int32)
    length_limit = jnp.where(position // SEQ == 0, seq_lengths[0], seq_lengths[1])
    keep_rows = position % SEQ < length_limit
    kept_grad = jnp.where(keep_rows[:, None], incoming, jnp.zeros_like(incoming))
    saved_values, saved_scale, saved_normed = norm_rows(saved_block, gain_cols)
    saved_rank = contract_last(saved_normed, down_rows)
    saved_act = jax.nn.silu(saved_rank).astype(jnp.bfloat16)
    rank_slope = contract_last(kept_grad, up_rows)
    back_rank = (rank_slope * silu_slope(saved_rank)).astype(jnp.bfloat16)
    back_normed = jnp.dot(back_rank, down_rows, preferred_element_type=jnp.float32)
    weighted = gain_cols * back_normed
    correction = lax.optimization_barrier(jnp.mean(saved_values * weighted, axis=1, keepdims=True))
    scale_cube = saved_scale * saved_scale * saved_scale
    grad_rows = (kept_grad.astype(jnp.float32) + saved_scale * weighted - saved_values * scale_cube * correction).astype(jnp.bfloat16)
    down_part = contract_rows(back_rank, saved_normed).astype(jnp.bfloat16)
    up_part = contract_rows(saved_act, kept_grad).astype(jnp.bfloat16)
    return (forward_out, grad_rows, down_part, up_part)

def section_tick(packed):
    forward_block, saved_block, incoming, seq_lengths, gain_row, down_rows, up_rows = packed
    gain_cols = gain_row.astype(jnp.float32)
    group_map = jax.vmap(group_tick, in_axes=(0, 0, 0, 0, None, None, None))
    forward_out, grad_rows, down_part, up_part = group_map(forward_block, saved_block, incoming, seq_lengths, gain_cols, down_rows, up_rows)
    down_part = lax.optimization_barrier(down_part)
    up_part = lax.optimization_barrier(up_part)
    mean_weight = 1.0 / N_DP
    grad_down = (lax.optimization_barrier(jnp.sum(down_part.astype(jnp.float32), axis=0)) * mean_weight).astype(jnp.bfloat16)
    grad_up = (lax.optimization_barrier(jnp.sum(up_part.astype(jnp.float32), axis=0)) * mean_weight).astype(jnp.bfloat16)
    return (forward_out, grad_rows, grad_down, grad_up)

def reference(forward_rows, saved_rows, output_grad, lengths, norm_gain, down_map, up_map):
    forward_out, grad_rows, grad_down, grad_up = lax.map(section_tick, (forward_rows, saved_rows, output_grad, lengths, norm_gain, down_map, up_map))
    next_inputs = jnp.concatenate([jnp.zeros_like(forward_out[:1]), forward_out[:-1]], axis=0)
    next_grads = jnp.concatenate([grad_rows[1:], jnp.zeros_like(grad_rows[:1])], axis=0)
    return (next_inputs, next_grads, grad_down, grad_up)
```

```python
import functools

import jax
import jax.numpy as jnp
from jax import lax
from jax.experimental import pallas as pl
from jax.experimental.pallas import tpu as pltpu
from jax.sharding import PartitionSpec as P

EPSILON = 1e-05
LANES = 128
F32 = jnp.float32
BF16 = jnp.bfloat16


def contract_last(left_side, right_side):
    return lax.dot_general(
        left_side, right_side, (((1,), (1,)), ((), ())), preferred_element_type=F32
    )


def contract_rows(left_side, right_side):
    return lax.dot_general(
        left_side, right_side, (((0,), (0,)), ((), ())), preferred_element_type=F32
    )


def flip(index, bit):
    step = 1 << bit
    return index + step * (1 - 2 * ((index // step) % 2))


def split_two(value):
    high = value.astype(BF16).astype(F32)
    return high, value - high


def tick(sizes, fwd_hbm, sav_hbm, grad_hbm, len_ref, gain_ref, down_hbm, up_hbm,
         next_in, next_gr, grad_down, grad_up,
         fwd, sav, kept, down, up, scaled,
         acc_f, acc_b, send_f, recv_f, send_b, recv_b, out_f, out_b,
         part, part_recv, load_sem,
         f_send_sem, f_recv_sem, b_send_sem, b_recv_sem,
         sec_send_sem, sec_recv_sem, dp_send_sem, dp_recv_sem):
    n_sec, n_ten, n_dp, chunk = sizes
    rows, width = fwd.shape
    rank = down.shape[0]
    full_width = width * n_ten
    n_seq = len_ref.shape[1]
    bits = n_ten.bit_length() - 1
    half = rows // 2
    n_chunk = width // chunk
    share = rank // n_dp
    sec, ten, dp = lax.axis_index("section"), lax.axis_index("tensor"), lax.axis_index("dp")

    loads = [
        pltpu.make_async_copy(src, dst, load_sem.at[i])
        for i, (src, dst) in enumerate(
            ((fwd_hbm, fwd), (down_hbm, down), (sav_hbm, sav), (grad_hbm, kept), (up_hbm, up))
        )
    ]
    for load in loads:
        load.start()

    barrier = pltpu.get_barrier_semaphore()
    for bit in range(bits):
        pl.semaphore_signal(barrier, inc=1, device_id={"tensor": flip(ten, bit)})
    for k in range(1, n_dp):
        pl.semaphore_signal(barrier, inc=1, device_id={"dp": (dp + k) % n_dp})

    @pl.when(sec > 0)
    def _():
        pl.semaphore_signal(barrier, inc=1, device_id={"section": sec - 1})

    @pl.when(sec < n_sec - 1)
    def _():
        pl.semaphore_signal(barrier, inc=1, device_id={"section": sec + 1})

    columns = [slice(c * chunk, (c + 1) * chunk) for c in range(n_chunk)]

    loads[0].wait()
    loads[1].wait()
    total = jnp.zeros((rows, rank), F32)
    square_f = jnp.zeros((rows, 1), F32)
    for cols in columns:
        values = fwd[:, cols].astype(F32)
        square_f += jnp.sum(values * values, axis=1, keepdims=True)
        gained = (values * gain_ref[:, cols].astype(F32)).astype(BF16)
        total += contract_last(gained, down[:, cols])
    loads[2].wait()
    square_s = jnp.zeros((rows, 1), F32)
    for cols in columns:
        values = sav[:, cols].astype(F32)
        square_s += jnp.sum(values * values, axis=1, keepdims=True)
        scaled[:, cols] = (values * gain_ref[:, cols].astype(F32)).astype(BF16)
    wide = acc_f.shape[1]
    packed = jnp.concatenate([total, jnp.zeros((rows, wide - rank), F32)], axis=1)
    lane = lax.broadcasted_iota(jnp.int32, (rows, wide), 1)
    for i, piece in enumerate(split_two(square_f) + split_two(square_s)):
        packed = jnp.where(lane == rank + i, piece, packed)
    acc_f[...] = packed

    pl.semaphore_wait(barrier, bits + n_dp - 1 + jnp.where(sec > 0, 1, 0) + jnp.where(sec < n_sec - 1, 1, 0))

    def exchange(send, recv, send_sem, recv_sem, h, p):
        span = pl.ds(h * half, half)
        return pltpu.make_async_remote_copy(
            src_ref=send.at[p, span],
            dst_ref=recv.at[p, span],
            send_sem=send_sem.at[h, p],
            recv_sem=recv_sem.at[h, p],
            device_id={"tensor": flip(ten, (h + p) % bits)},
        )

    forms = ((acc_f, send_f, recv_f, f_send_sem, f_recv_sem), (acc_b, send_b, recv_b, b_send_sem, b_recv_sem))

    def begin(form, p):
        acc, send, recv, send_sem, recv_sem = form
        for h in range(2):
            span = pl.ds(h * half, half)
            send[p, span] = acc[span].astype(BF16)
            exchange(send, recv, send_sem, recv_sem, h, p).start()

    def finish(form, p):
        acc, send, recv, send_sem, recv_sem = form
        for h in range(2):
            span = pl.ds(h * half, half)
            exchange(send, recv, send_sem, recv_sem, h, p).wait()
            acc[span] = acc[span] + recv[p, span].astype(F32)

    if bits:
        begin(forms[0], 0)

    total_s = jnp.zeros((rows, rank), F32)
    for cols in columns:
        total_s += contract_last(scaled[:, cols], down[:, cols])
    loads[3].wait()
    loads[4].wait()
    position = lax.broadcasted_iota(jnp.int32, (rows, 1), 0)
    seq_rows = rows // n_seq
    limit = jnp.full((rows, 1), 0, jnp.int32)
    for i in range(n_seq):
        limit = jnp.where(position >= i * seq_rows, i * seq_rows + len_ref[0, i], limit)
    keep = position < limit
    total_g = jnp.zeros((rows, rank), F32)
    for cols in columns:
        held = jnp.where(keep, kept[:, cols].astype(F32), 0.0).astype(BF16)
        kept[:, cols] = held
        total_g += contract_last(held, up[:, cols])
    acc_b[...] = jnp.concatenate([total_g, total_s], axis=1)
    if bits:
        begin(forms[1], 0)
    for p in range(1, bits):
        for form in forms:
            finish(form, p - 1)
            begin(form, p)
    if bits:
        finish(forms[0], bits - 1)

    lane = lax.broadcasted_iota(jnp.int32, (rows, wide), 1)
    reduced = acc_f[...]
    square_f = jnp.sum(jnp.where((lane == rank) | (lane == rank + 1), reduced, 0.0), axis=1, keepdims=True)
    square_s = jnp.sum(jnp.where((lane == rank + 2) | (lane == rank + 3), reduced, 0.0), axis=1, keepdims=True)
    scale_f = lax.rsqrt(square_f / full_width + EPSILON)
    scale_s = lax.rsqrt(square_s / full_width + EPSILON)

    def shift(way, source, target, c):
        span = pl.ds(c * chunk, chunk)
        return pltpu.make_async_remote_copy(
            src_ref=source.at[:, span],
            dst_ref=target.at[:, span],
            send_sem=sec_send_sem.at[way, c],
            recv_sem=sec_recv_sem.at[way, c],
            device_id={"section": sec + 1 if way == 0 else sec - 1},
        )

    rank_f = reduced[:, :rank] * scale_f
    act_f = (rank_f * jax.nn.sigmoid(rank_f)).astype(BF16)

    @pl.when(sec < n_sec - 1)
    def _():
        for c, cols in enumerate(columns):
            grown = jnp.dot(act_f, up[:, cols], preferred_element_type=F32)
            out_f[:, cols] = (fwd[:, cols].astype(F32) + grown).astype(BF16)
            shift(0, out_f, next_in, c).start()

    if bits:
        finish(forms[1], bits - 1)
    slope = acc_b[:, :rank]
    rank_s = acc_b[:, rank:] * scale_s
    gate = jax.nn.sigmoid(rank_s)
    act_s = (rank_s * gate).astype(BF16)
    back = slope * (gate * (1.0 + rank_s * (1.0 - gate)))
    back_b = back.astype(BF16)
    tilt = jnp.sum(back_b.astype(F32) * rank_s, axis=1, keepdims=True) * (scale_s * scale_s / full_width)

    @pl.when(sec > 0)
    def _():
        for c, cols in enumerate(columns):
            normed = jnp.dot(back_b, down[:, cols], preferred_element_type=F32)
            out_b[:, cols] = (
                kept[:, cols].astype(F32)
                + scale_s * (gain_ref[:, cols].astype(F32) * normed)
                - sav[:, cols].astype(F32) * tilt
            ).astype(BF16)
            shift(1, out_b, next_gr, c).start()

    back_scaled = (back * scale_s).astype(BF16)

    def trade(i, k):
        target = (dp + k) % n_dp
        return pltpu.make_async_remote_copy(
            src_ref=part.at[i, pl.ds(pl.multiple_of(target * share, share), share)],
            dst_ref=part_recv.at[i, k - 1],
            send_sem=dp_send_sem.at[i, k - 1],
            recv_sem=dp_recv_sem.at[i, k - 1],
            device_id={"dp": target},
        )

    for i, (left_side, right_side) in enumerate(((back_scaled, scaled), (act_s, kept))):
        for cols in columns:
            part[i, :, cols] = contract_rows(left_side, right_side[:, cols]).astype(BF16)
        for k in range(1, n_dp):
            trade(i, k).start()
    mine = pl.ds(pl.multiple_of(dp * share, share), share)
    for i, out in enumerate((grad_down, grad_up)):
        for k in range(1, n_dp):
            trade(i, k).wait()
        for cols in columns:
            summed = part[i, mine, cols].astype(F32)
            for k in range(1, n_dp):
                summed += part_recv[i, k - 1, :, cols].astype(F32)
            out[:, cols] = (summed * (1.0 / n_dp)).astype(BF16)

    @pl.when(sec == 0)
    def _():
        next_in[...] = jnp.zeros_like(next_in)

    @pl.when(sec == n_sec - 1)
    def _():
        next_gr[...] = jnp.zeros_like(next_gr)

    for c in range(n_chunk):
        @pl.when(sec < n_sec - 1)
        def _():
            shift(0, out_f, next_in, c).wait_send()
            shift(1, out_b, next_gr, c).wait_recv()

        @pl.when(sec > 0)
        def _():
            shift(1, out_b, next_gr, c).wait_send()
            shift(0, out_f, next_in, c).wait_recv()


def solution(mesh):
    n_sec, n_ten, n_dp = (mesh.shape[name] for name in ("section", "tensor", "dp"))

    def shards(forward_rows, saved_rows, output_grad, lengths, norm_gain, down_map, up_map):
        rows, width = forward_rows.shape[2:]
        rank = down_map.shape[1]
        share = rank // n_dp
        bits = n_ten.bit_length() - 1
        chunk = min(width, 4 * LANES)
        n_chunk = width // chunk
        wide = -(-(rank + 4) // LANES) * LANES
        steps = max(bits, 1)
        vmem = pl.BlockSpec(memory_space=pltpu.VMEM)
        anywhere = pl.BlockSpec(memory_space=pl.ANY)
        flops = 7 * 2 * rows * rank * width
        dma = pltpu.SemaphoreType.DMA
        results = pl.pallas_call(
            functools.partial(tick, (n_sec, n_ten, n_dp, chunk)),
            out_shape=(
                jax.ShapeDtypeStruct((rows, width), BF16),
                jax.ShapeDtypeStruct((rows, width), BF16),
                jax.ShapeDtypeStruct((share, width), BF16),
                jax.ShapeDtypeStruct((share, width), BF16),
            ),
            in_specs=[anywhere, anywhere, anywhere, pl.BlockSpec(memory_space=pltpu.SMEM), vmem, anywhere, anywhere],
            out_specs=(vmem,) * 4,
            scratch_shapes=[
                pltpu.VMEM((rows, width), BF16),
                pltpu.VMEM((rows, width), BF16),
                pltpu.VMEM((rows, width), BF16),
                pltpu.VMEM((rank, width), BF16),
                pltpu.VMEM((rank, width), BF16),
                pltpu.VMEM((rows, width), BF16),
                pltpu.VMEM((rows, wide), F32),
                pltpu.VMEM((rows, 2 * rank), F32),
                pltpu.VMEM((steps, rows, wide), BF16),
                pltpu.VMEM((steps, rows, wide), BF16),
                pltpu.VMEM((steps, rows, 2 * rank), BF16),
                pltpu.VMEM((steps, rows, 2 * rank), BF16),
                pltpu.VMEM((rows, width), BF16),
                pltpu.VMEM((rows, width), BF16),
                pltpu.VMEM((2, rank, width), BF16),
                pltpu.VMEM((2, max(n_dp - 1, 1), share, width), BF16),
                dma((5,)),
                dma((2, steps)),
                dma((2, steps)),
                dma((2, steps)),
                dma((2, steps)),
                dma((2, n_chunk)),
                dma((2, n_chunk)),
                dma((2, max(n_dp - 1, 1))),
                dma((2, max(n_dp - 1, 1))),
            ],
            compiler_params=pltpu.CompilerParams(collective_id=0, has_side_effects=True),
            cost_estimate=pl.CostEstimate(
                flops=flops, bytes_accessed=16 * rows * width, transcendentals=4 * rows * rank
            ),
            name="tick",
        )(
            forward_rows[0, 0], saved_rows[0, 0], output_grad[0, 0], lengths[0], norm_gain, down_map[0], up_map[0]
        )
        next_inputs, next_grads, grad_down, grad_up = results
        return next_inputs[None, None], next_grads[None, None], grad_down[None], grad_up[None]

    row_spec = P("section", "dp", None, "tensor")
    map_spec = P("section", None, "tensor")
    part_spec = P("section", "dp", "tensor")
    return jax.shard_map(
        shards,
        mesh=mesh,
        in_specs=(row_spec, row_spec, row_spec, P("section", "dp"), P("section", "tensor"), map_spec, map_spec),
        out_specs=(row_spec, row_spec, part_spec, part_spec),
        check_vma=False,
    )
```

```python
import functools

import jax
import jax.numpy as jnp
from jax import lax
from jax.experimental import pallas as pl
from jax.experimental.pallas import tpu as pltpu
from jax.sharding import PartitionSpec as P

EPSILON = 1e-05
LANES = 128
F32 = jnp.float32
BF16 = jnp.bfloat16


def contract_last(left_side, right_side):
    return lax.dot_general(
        left_side, right_side, (((1,), (1,)), ((), ())), preferred_element_type=F32
    )


def contract_rows(left_side, right_side):
    return lax.dot_general(
        left_side, right_side, (((0,), (0,)), ((), ())), preferred_element_type=F32
    )


def flip(index, bit):
    step = 1 << bit
    return index + step * (1 - 2 * ((index // step) % 2))


def split_two(value):
    high = value.astype(BF16).astype(F32)
    return high, value - high


def tick(sizes, fwd_hbm, sav_hbm, grad_hbm, len_ref, gain_ref, down_hbm, up_hbm,
         next_in, next_gr, grad_down, grad_up,
         fwd, sav, kept, down, up, scaled,
         acc_f, acc_b, send_f, recv_f, send_b, recv_b, out_f, out_b,
         part, part_recv, load_sem,
         f_send_sem, f_recv_sem, b_send_sem, b_recv_sem,
         sec_send_sem, sec_recv_sem, dp_send_sem, dp_recv_sem):
    n_sec, n_ten, n_dp, chunk = sizes
    rows, width = fwd.shape
    rank = down.shape[0]
    full_width = width * n_ten
    n_seq = len_ref.shape[1]
    bits = n_ten.bit_length() - 1
    half = rows // 2
    n_chunk = width // chunk
    share = rank // n_dp
    sec, ten, dp = lax.axis_index("section"), lax.axis_index("tensor"), lax.axis_index("dp")

    loads = [
        pltpu.make_async_copy(src, dst, load_sem.at[i])
        for i, (src, dst) in enumerate(
            ((fwd_hbm, fwd), (down_hbm, down), (sav_hbm, sav), (grad_hbm, kept), (up_hbm, up))
        )
    ]
    for load in loads:
        load.start()

    barrier = pltpu.get_barrier_semaphore()
    for bit in range(bits):
        pl.semaphore_signal(barrier, inc=1, device_id={"tensor": flip(ten, bit)})
    for k in range(1, n_dp):
        pl.semaphore_signal(barrier, inc=1, device_id={"dp": (dp + k) % n_dp})

    @pl.when(sec > 0)
    def _():
        pl.semaphore_signal(barrier, inc=1, device_id={"section": sec - 1})

    @pl.when(sec < n_sec - 1)
    def _():
        pl.semaphore_signal(barrier, inc=1, device_id={"section": sec + 1})

    columns = [slice(c * chunk, (c + 1) * chunk) for c in range(n_chunk)]

    loads[0].wait()
    loads[1].wait()
    total = jnp.zeros((rows, rank), F32)
    square_f = jnp.zeros((rows, 1), F32)
    for cols in columns:
        values = fwd[:, cols].astype(F32)
        square_f += jnp.sum(values * values, axis=1, keepdims=True)
        gained = (values * gain_ref[:, cols].astype(F32)).astype(BF16)
        total += contract_last(gained, down[:, cols])
    loads[2].wait()
    square_s = jnp.zeros((rows, 1), F32)
    for cols in columns:
        values = sav[:, cols].astype(F32)
        square_s += jnp.sum(values * values, axis=1, keepdims=True)
        scaled[:, cols] = (values * gain_ref[:, cols].astype(F32)).astype(BF16)
    wide = acc_f.shape[1]
    packed = jnp.concatenate([total, jnp.zeros((rows, wide - rank), F32)], axis=1)
    lane = lax.broadcasted_iota(jnp.int32, (rows, wide), 1)
    for i, piece in enumerate(split_two(square_f) + split_two(square_s)):
        packed = jnp.where(lane == rank + i, piece, packed)
    acc_f[...] = packed

    pl.semaphore_wait(barrier, bits + n_dp - 1 + jnp.where(sec > 0, 1, 0) + jnp.where(sec < n_sec - 1, 1, 0))

    def exchange(send, recv, send_sem, recv_sem, h, p):
        span = pl.ds(h * half, half)
        return pltpu.make_async_remote_copy(
            src_ref=send.at[p, span],
            dst_ref=recv.at[p, span],
            send_sem=send_sem.at[h, p],
            recv_sem=recv_sem.at[h, p],
            device_id={"tensor": flip(ten, (h + p) % bits)},
        )

    forms = ((acc_f, send_f, recv_f, f_send_sem, f_recv_sem), (acc_b, send_b, recv_b, b_send_sem, b_recv_sem))

    def begin(form, p):
        acc, send, recv, send_sem, recv_sem = form
        for h in range(2):
            span = pl.ds(h * half, half)
            send[p, span] = acc[span].astype(BF16)
            exchange(send, recv, send_sem, recv_sem, h, p).start()

    def finish(form, p):
        acc, send, recv, send_sem, recv_sem = form
        for h in range(2):
            span = pl.ds(h * half, half)
            exchange(send, recv, send_sem, recv_sem, h, p).wait()
            acc[span] = acc[span] + recv[p, span].astype(F32)

    if bits:
        begin(forms[0], 0)

    total_s = jnp.zeros((rows, rank), F32)
    for cols in columns:
        total_s += contract_last(scaled[:, cols], down[:, cols])
    loads[3].wait()
    loads[4].wait()
    position = lax.broadcasted_iota(jnp.int32, (rows, 1), 0)
    seq_rows = rows // n_seq
    limit = jnp.full((rows, 1), 0, jnp.int32)
    for i in range(n_seq):
        limit = jnp.where(position >= i * seq_rows, i * seq_rows + len_ref[0, i], limit)
    keep = position < limit
    total_g = jnp.zeros((rows, rank), F32)
    for cols in columns:
        held = jnp.where(keep, kept[:, cols].astype(F32), 0.0).astype(BF16)
        kept[:, cols] = held
        total_g += contract_last(held, up[:, cols])
    acc_b[...] = jnp.concatenate([total_g, total_s], axis=1)
    if bits:
        begin(forms[1], 0)
    for p in range(1, bits):
        for form in forms:
            finish(form, p - 1)
            begin(form, p)
    if bits:
        finish(forms[0], bits - 1)

    lane = lax.broadcasted_iota(jnp.int32, (rows, wide), 1)
    reduced = acc_f[...]
    square_f = jnp.sum(jnp.where((lane == rank) | (lane == rank + 1), reduced, 0.0), axis=1, keepdims=True)
    square_s = jnp.sum(jnp.where((lane == rank + 2) | (lane == rank + 3), reduced, 0.0), axis=1, keepdims=True)
    scale_f = lax.rsqrt(square_f / full_width + EPSILON)
    scale_s = lax.rsqrt(square_s / full_width + EPSILON)

    def shift(way, source, target, c):
        span = pl.ds(c * chunk, chunk)
        return pltpu.make_async_remote_copy(
            src_ref=source.at[:, span],
            dst_ref=target.at[:, span],
            send_sem=sec_send_sem.at[way, c],
            recv_sem=sec_recv_sem.at[way, c],
            device_id={"section": sec + 1 if way == 0 else sec - 1},
        )

    rank_f = reduced[:, :rank] * scale_f
    act_f = (rank_f * jax.nn.sigmoid(rank_f)).astype(BF16)

    @pl.when(sec < n_sec - 1)
    def _():
        for c, cols in enumerate(columns):
            grown = jnp.dot(act_f, up[:, cols], preferred_element_type=F32)
            out_f[:, cols] = (fwd[:, cols].astype(F32) + grown).astype(BF16)
            shift(0, out_f, next_in, c).start()

    if bits:
        finish(forms[1], bits - 1)
    slope = acc_b[:, :rank]
    rank_s = acc_b[:, rank:] * scale_s
    gate = jax.nn.sigmoid(rank_s)
    act_s = (rank_s * gate).astype(BF16)
    back = slope * (gate * (1.0 + rank_s * (1.0 - gate)))
    back_b = back.astype(BF16)
    tilt = jnp.sum(back_b.astype(F32) * rank_s, axis=1, keepdims=True) * (scale_s * scale_s / full_width)

    @pl.when(sec > 0)
    def _():
        for c, cols in enumerate(columns):
            normed = jnp.dot(back_b, down[:, cols], preferred_element_type=F32)
            out_b[:, cols] = (
                kept[:, cols].astype(F32)
                + scale_s * (gain_ref[:, cols].astype(F32) * normed)
                - sav[:, cols].astype(F32) * tilt
            ).astype(BF16)
            shift(1, out_b, next_gr, c).start()

    back_scaled = (back * scale_s).astype(BF16)

    def trade(i, k):
        target = (dp + k) % n_dp
        return pltpu.make_async_remote_copy(
            src_ref=part.at[i, pl.ds(pl.multiple_of(target * share, share), share)],
            dst_ref=part_recv.at[i, k - 1],
            send_sem=dp_send_sem.at[i, k - 1],
            recv_sem=dp_recv_sem.at[i, k - 1],
            device_id={"dp": target},
        )

    for i, (left_side, right_side) in enumerate(((back_scaled, scaled), (act_s, kept))):
        for cols in columns:
            part[i, :, cols] = contract_rows(left_side, right_side[:, cols]).astype(BF16)
        for k in range(1, n_dp):
            trade(i, k).start()
    mine = pl.ds(pl.multiple_of(dp * share, share), share)
    for i, out in enumerate((grad_down, grad_up)):
        for k in range(1, n_dp):
            trade(i, k).wait()
        for cols in columns:
            summed = part[i, mine, cols].astype(F32)
            for k in range(1, n_dp):
                summed += part_recv[i, k - 1, :, cols].astype(F32)
            out[:, cols] = (summed * (1.0 / n_dp)).astype(BF16)

    @pl.when(sec == 0)
    def _():
        next_in[...] = jnp.zeros_like(next_in)

    @pl.when(sec == n_sec - 1)
    def _():
        next_gr[...] = jnp.zeros_like(next_gr)

    for c in range(n_chunk):
        @pl.when(sec < n_sec - 1)
        def _():
            shift(0, out_f, next_in, c).wait_send()
            shift(1, out_b, next_gr, c).wait_recv()

        @pl.when(sec > 0)
        def _():
            shift(1, out_b, next_gr, c).wait_send()
            shift(0, out_f, next_in, c).wait_recv()


def place(*refs):
    count = len(refs) // 2
    sems = refs[-1]
    copies = [pltpu.make_async_copy(refs[i], refs[count + i], sems.at[i]) for i in range(count)]
    for copy in copies:
        copy.start()
    for copy in copies:
        copy.wait()


def solution(mesh):
    n_sec, n_ten, n_dp = (mesh.shape[name] for name in ("section", "tensor", "dp"))

    def shards(forward_rows, saved_rows, output_grad, lengths, norm_gain, down_map, up_map):
        rows, width = forward_rows.shape[2:]
        rank = down_map.shape[1]
        share = rank // n_dp
        bits = n_ten.bit_length() - 1
        chunk = min(width, 4 * LANES)
        n_chunk = width // chunk
        wide = -(-(rank + 4) // LANES) * LANES
        steps = max(bits, 1)
        vmem = pl.BlockSpec(memory_space=pltpu.VMEM)
        anywhere = pl.BlockSpec(memory_space=pl.ANY)
        flops = 7 * 2 * rows * rank * width
        dma = pltpu.SemaphoreType.DMA
        shapes = ((rows, width),) * 2 + ((share, width),) * 2
        results = pl.pallas_call(
            functools.partial(tick, (n_sec, n_ten, n_dp, chunk)),
            out_shape=tuple(pltpu.VMEM(shape, BF16) for shape in shapes),
            in_specs=[anywhere, anywhere, anywhere, pl.BlockSpec(memory_space=pltpu.SMEM), vmem, anywhere, anywhere],
            out_specs=(vmem,) * 4,
            scratch_shapes=[
                pltpu.VMEM((rows, width), BF16),
                pltpu.VMEM((rows, width), BF16),
                pltpu.VMEM((rows, width), BF16),
                pltpu.VMEM((rank, width), BF16),
                pltpu.VMEM((rank, width), BF16),
                pltpu.VMEM((rows, width), BF16),
                pltpu.VMEM((rows, wide), F32),
                pltpu.VMEM((rows, 2 * rank), F32),
                pltpu.VMEM((steps, rows, wide), BF16),
                pltpu.VMEM((steps, rows, wide), BF16),
                pltpu.VMEM((steps, rows, 2 * rank), BF16),
                pltpu.VMEM((steps, rows, 2 * rank), BF16),
                pltpu.VMEM((rows, width), BF16),
                pltpu.VMEM((rows, width), BF16),
                pltpu.VMEM((2, rank, width), BF16),
                pltpu.VMEM((2, max(n_dp - 1, 1), share, width), BF16),
                dma((5,)),
                dma((2, steps)),
                dma((2, steps)),
                dma((2, steps)),
                dma((2, steps)),
                dma((2, n_chunk)),
                dma((2, n_chunk)),
                dma((2, max(n_dp - 1, 1))),
                dma((2, max(n_dp - 1, 1))),
            ],
            compiler_params=pltpu.CompilerParams(collective_id=0, has_side_effects=True),
            cost_estimate=pl.CostEstimate(
                flops=flops, bytes_accessed=16 * rows * width, transcendentals=4 * rows * rank
            ),
            name="tick",
        )(
            forward_rows[0, 0], saved_rows[0, 0], output_grad[0, 0], lengths[0], norm_gain, down_map[0], up_map[0]
        )
        next_inputs, next_grads, grad_down, grad_up = pl.pallas_call(
            place,
            out_shape=tuple(jax.ShapeDtypeStruct(shape, BF16) for shape in shapes),
            in_specs=[vmem] * 4,
            out_specs=(anywhere,) * 4,
            scratch_shapes=[dma((4,))],
            name="place",
        )(*[pltpu.with_memory_space_constraint(x, pltpu.VMEM) for x in results])
        return next_inputs[None, None], next_grads[None, None], grad_down[None], grad_up[None]

    row_spec = P("section", "dp", None, "tensor")
    map_spec = P("section", None, "tensor")
    part_spec = P("section", "dp", "tensor")
    return jax.shard_map(
        shards,
        mesh=mesh,
        in_specs=(row_spec, row_spec, row_spec, P("section", "dp"), P("section", "tensor"), map_spec, map_spec),
        out_specs=(row_spec, row_spec, part_spec, part_spec),
        check_vma=False,
    )
```

```python
import functools

import jax
import jax.numpy as jnp
from jax import lax
from jax.experimental import pallas as pl
from jax.experimental.pallas import tpu as pltpu
from jax.sharding import PartitionSpec as P

EPSILON = 1e-05
LANES = 128
RAW_FORWARD = 0.375
RAW_BACK = 0.25
F32 = jnp.float32
BF16 = jnp.bfloat16


def contract_last(left_side, right_side):
    return lax.dot_general(
        left_side, right_side, (((1,), (1,)), ((), ())), preferred_element_type=F32
    )


def contract_rows(left_side, right_side):
    return lax.dot_general(
        left_side, right_side, (((0,), (0,)), ((), ())), preferred_element_type=F32
    )


def flip(index, bit):
    step = 1 << bit
    return index + step * (1 - 2 * ((index // step) % 2))


def split_two(value):
    high = value.astype(BF16).astype(F32)
    return high, value - high


def tick(sizes, fwd_hbm, sav_hbm, grad_hbm, len_ref, gain_ref, down_hbm, up_hbm,
         next_in, next_gr, grad_down, grad_up,
         fwd, sav, kept, down, up, scaled,
         acc_f, acc_b, send_f, recv_f, send_b, recv_b, out_f, out_b,
         part, part_recv, act_out, act_in, back_out, back_in,
         raw_fwd, raw_up, raw_sav, raw_grad, raw_down, raw_gain, load_sem,
         f_send_sem, f_recv_sem, b_send_sem, b_recv_sem,
         sec_send_sem, sec_recv_sem, dp_send_sem, dp_recv_sem,
         raw_send_sem, raw_recv_sem, relay_send_sem, relay_recv_sem):
    n_sec, n_ten, n_dp, chunk = sizes
    rows, width = fwd.shape
    rank = down.shape[0]
    full_width = width * n_ten
    n_seq = len_ref.shape[1]
    bits = n_ten.bit_length() - 1
    half = rows // 2
    n_chunk = width // chunk
    share = rank // n_dp
    sec, ten, dp = lax.axis_index("section"), lax.axis_index("tensor"), lax.axis_index("dp")

    loads = [
        pltpu.make_async_copy(src, dst, load_sem.at[i])
        for i, (src, dst) in enumerate(
            ((fwd_hbm, fwd), (down_hbm, down), (sav_hbm, sav), (grad_hbm, kept), (up_hbm, up))
        )
    ]
    for load in loads:
        load.start()

    barrier = pltpu.get_barrier_semaphore()
    for bit in range(bits):
        pl.semaphore_signal(barrier, inc=1, device_id={"tensor": flip(ten, bit)})
    for k in range(1, n_dp):
        pl.semaphore_signal(barrier, inc=1, device_id={"dp": (dp + k) % n_dp})

    @pl.when(sec > 0)
    def _():
        pl.semaphore_signal(barrier, inc=1, device_id={"section": sec - 1})

    @pl.when(sec < n_sec - 1)
    def _():
        pl.semaphore_signal(barrier, inc=1, device_id={"section": sec + 1})

    columns = [slice(c * chunk, (c + 1) * chunk) for c in range(n_chunk)]
    raw_f, raw_b = raw_fwd.shape[1], raw_sav.shape[1]
    mine = pl.ds(pl.multiple_of(dp * share, share), share)
    tail_f, tail_b = pl.ds(width - raw_f, raw_f), pl.ds(width - raw_b, raw_b)

    def across(i, source, target, step):
        return pltpu.make_async_remote_copy(
            src_ref=source,
            dst_ref=target,
            send_sem=raw_send_sem.at[i],
            recv_sem=raw_recv_sem.at[i],
            device_id={"section": sec + step},
        )

    raw_ups = across(0, up_hbm.at[mine, tail_f], raw_up.at[mine], 1)
    raw_fwds = across(1, fwd_hbm.at[:, tail_f], raw_fwd, 1)
    acts = across(2, act_out, act_in, 1)
    raw_downs = across(3, down_hbm.at[mine, tail_b], raw_down.at[mine], -1)
    raw_gains = across(4, gain_ref, raw_gain, -1)
    raw_savs = across(5, sav_hbm.at[:, tail_b], raw_sav, -1)
    raw_grads = across(6, grad_hbm.at[:, tail_b], raw_grad, -1)
    backs = across(7, back_out, back_in, -1)
    up_way, down_way = (raw_ups, raw_fwds, acts), (raw_downs, raw_gains, raw_savs, raw_grads, backs)

    def relay(way, k):
        ref = (raw_up, raw_down)[way].at[mine]
        return pltpu.make_async_remote_copy(
            src_ref=ref,
            dst_ref=ref,
            send_sem=relay_send_sem.at[way, k - 1],
            recv_sem=relay_recv_sem.at[way, k - 1],
            device_id={"dp": (dp + k) % n_dp},
        )

    pl.semaphore_wait(barrier, bits + n_dp - 1 + jnp.where(sec > 0, 1, 0) + jnp.where(sec < n_sec - 1, 1, 0))

    @pl.when(sec < n_sec - 1)
    def _():
        for copy in up_way[:-1]:
            copy.start()

    @pl.when(sec > 0)
    def _():
        for copy in down_way[:-1]:
            copy.start()

    loads[0].wait()
    loads[1].wait()
    total = jnp.zeros((rows, rank), F32)
    square_f = jnp.zeros((rows, 1), F32)
    for cols in columns:
        values = fwd[:, cols].astype(F32)
        square_f += jnp.sum(values * values, axis=1, keepdims=True)
        gained = (values * gain_ref[:, cols].astype(F32)).astype(BF16)
        total += contract_last(gained, down[:, cols])
    loads[2].wait()
    square_s = jnp.zeros((rows, 1), F32)
    for cols in columns:
        values = sav[:, cols].astype(F32)
        square_s += jnp.sum(values * values, axis=1, keepdims=True)
        scaled[:, cols] = (values * gain_ref[:, cols].astype(F32)).astype(BF16)
    wide = acc_f.shape[1]
    packed = jnp.concatenate([total, jnp.zeros((rows, wide - rank), F32)], axis=1)
    lane = lax.broadcasted_iota(jnp.int32, (rows, wide), 1)
    for i, piece in enumerate(split_two(square_f) + split_two(square_s)):
        packed = jnp.where(lane == rank + i, piece, packed)
    acc_f[...] = packed

    def exchange(send, recv, send_sem, recv_sem, h, p):
        span = pl.ds(h * half, half)
        return pltpu.make_async_remote_copy(
            src_ref=send.at[p, span],
            dst_ref=recv.at[p, span],
            send_sem=send_sem.at[h, p],
            recv_sem=recv_sem.at[h, p],
            device_id={"tensor": flip(ten, (h + p) % bits)},
        )

    forms = ((acc_f, send_f, recv_f, f_send_sem, f_recv_sem), (acc_b, send_b, recv_b, b_send_sem, b_recv_sem))

    def begin(form, p):
        acc, send, recv, send_sem, recv_sem = form
        for h in range(2):
            span = pl.ds(h * half, half)
            send[p, span] = acc[span].astype(BF16)
            exchange(send, recv, send_sem, recv_sem, h, p).start()

    def finish(form, p):
        acc, send, recv, send_sem, recv_sem = form
        for h in range(2):
            span = pl.ds(h * half, half)
            exchange(send, recv, send_sem, recv_sem, h, p).wait()
            acc[span] = acc[span] + recv[p, span].astype(F32)

    if bits:
        begin(forms[0], 0)

    total_s = jnp.zeros((rows, rank), F32)
    for cols in columns:
        total_s += contract_last(scaled[:, cols], down[:, cols])
    loads[3].wait()
    loads[4].wait()
    position = lax.broadcasted_iota(jnp.int32, (rows, 1), 0)
    seq_rows = rows // n_seq
    limit = jnp.full((rows, 1), 0, jnp.int32)
    for i in range(n_seq):
        limit = jnp.where(position >= i * seq_rows, i * seq_rows + len_ref[0, i], limit)
    keep = position < limit
    total_g = jnp.zeros((rows, rank), F32)
    for cols in columns:
        held = jnp.where(keep, kept[:, cols].astype(F32), 0.0).astype(BF16)
        kept[:, cols] = held
        total_g += contract_last(held, up[:, cols])
    acc_b[...] = jnp.concatenate([total_g, total_s], axis=1)
    if bits:
        begin(forms[1], 0)
    for p in range(1, bits):
        for form in forms:
            finish(form, p - 1)
            begin(form, p)
    if bits:
        finish(forms[0], bits - 1)

    lane = lax.broadcasted_iota(jnp.int32, (rows, wide), 1)
    reduced = acc_f[...]
    square_f = jnp.sum(jnp.where((lane == rank) | (lane == rank + 1), reduced, 0.0), axis=1, keepdims=True)
    square_s = jnp.sum(jnp.where((lane == rank + 2) | (lane == rank + 3), reduced, 0.0), axis=1, keepdims=True)
    scale_f = lax.rsqrt(square_f / full_width + EPSILON)
    scale_s = lax.rsqrt(square_s / full_width + EPSILON)

    done_f = [slice(a, min(a + chunk, width - raw_f)) for a in range(0, width - raw_f, chunk)]
    done_b = [slice(a, min(a + chunk, width - raw_b)) for a in range(0, width - raw_b, chunk)]

    def shift(way, source, target, c):
        cols = (done_f, done_b)[way][c]
        span = pl.ds(cols.start, cols.stop - cols.start)
        return pltpu.make_async_remote_copy(
            src_ref=source.at[:, span],
            dst_ref=target.at[:, span],
            send_sem=sec_send_sem.at[way, c],
            recv_sem=sec_recv_sem.at[way, c],
            device_id={"section": sec + 1 if way == 0 else sec - 1},
        )

    rank_f = reduced[:, :rank] * scale_f
    act_f = rank_f * jax.nn.sigmoid(rank_f)

    @pl.when(sec < n_sec - 1)
    def _():
        act_out[...] = jnp.concatenate([act_f[:half], act_f[half:]], axis=1).astype(BF16)
        acts.start()

    act_f = act_f.astype(BF16)

    @pl.when(sec < n_sec - 1)
    def _():
        for c, cols in enumerate(done_f):
            grown = jnp.dot(act_f, up[:, cols], preferred_element_type=F32)
            out_f[:, cols] = (fwd[:, cols].astype(F32) + grown).astype(BF16)
            shift(0, out_f, next_in, c).start()

    if bits:
        finish(forms[1], bits - 1)
    slope = acc_b[:, :rank]
    rank_s = acc_b[:, rank:] * scale_s
    gate = jax.nn.sigmoid(rank_s)
    act_s = (rank_s * gate).astype(BF16)
    back = slope * (gate * (1.0 + rank_s * (1.0 - gate)))
    back_b = back.astype(BF16)
    tilt = jnp.sum(back_b.astype(F32) * rank_s, axis=1, keepdims=True) * (scale_s * scale_s / full_width)

    back_s = back * scale_s
    back_scaled = back_s.astype(BF16)

    @pl.when(sec > 0)
    def _():
        message = jnp.concatenate([back_s, jnp.zeros((rows, wide - rank), F32)], axis=1)
        for i, piece in enumerate(split_two(tilt) + (jnp.where(keep, 1.0, 0.0),)):
            message = jnp.where(lane == rank + i, piece, message)
        back_out[...] = message.astype(BF16)
        backs.start()
        for c, cols in enumerate(done_b):
            normed = jnp.dot(back_scaled, down[:, cols], preferred_element_type=F32)
            out_b[:, cols] = (
                kept[:, cols].astype(F32)
                + gain_ref[:, cols].astype(F32) * normed
                - sav[:, cols].astype(F32) * tilt
            ).astype(BF16)
            shift(1, out_b, next_gr, c).start()

    def trade(i, k):
        target = (dp + k) % n_dp
        return pltpu.make_async_remote_copy(
            src_ref=part.at[i, pl.ds(pl.multiple_of(target * share, share), share)],
            dst_ref=part_recv.at[i, k - 1],
            send_sem=dp_send_sem.at[i, k - 1],
            recv_sem=dp_recv_sem.at[i, k - 1],
            device_id={"dp": target},
        )

    for i, (left_side, right_side) in enumerate(((back_scaled, scaled), (act_s, kept))):
        for cols in columns:
            part[i, :, cols] = contract_rows(left_side, right_side[:, cols]).astype(BF16)
        for k in range(1, n_dp):
            trade(i, k).start()

    @pl.when(sec > 0)
    def _():
        raw_ups.wait_recv()
        for k in range(1, n_dp):
            relay(0, k).start()

    @pl.when(sec < n_sec - 1)
    def _():
        raw_downs.wait_recv()
        for k in range(1, n_dp):
            relay(1, k).start()

    for i, out in enumerate((grad_down, grad_up)):
        for k in range(1, n_dp):
            trade(i, k).wait()
        for cols in columns:
            summed = part[i, mine, cols].astype(F32)
            for k in range(1, n_dp):
                summed += part_recv[i, k - 1, :, cols].astype(F32)
            out[:, cols] = (summed * (1.0 / n_dp)).astype(BF16)

    @pl.when(sec == 0)
    def _():
        next_in[...] = jnp.zeros_like(next_in)

    @pl.when(sec == n_sec - 1)
    def _():
        next_gr[...] = jnp.zeros_like(next_gr)

    @pl.when(sec > 0)
    def _():
        for k in range(1, n_dp):
            relay(0, k).wait()
        raw_fwds.wait_recv()
        acts.wait_recv()
        came = act_in[...].astype(F32)
        came = jnp.concatenate([came[:, :rank], came[:, rank:]], axis=0).astype(BF16)
        for a in range(0, raw_f, chunk):
            b = min(a + chunk, raw_f)
            grown = jnp.dot(came, raw_up[:, a:b], preferred_element_type=F32)
            next_in[:, width - raw_f + a:width - raw_f + b] = (raw_fwd[:, a:b].astype(F32) + grown).astype(BF16)

    @pl.when(sec < n_sec - 1)
    def _():
        for k in range(1, n_dp):
            relay(1, k).wait()
        raw_gains.wait_recv()
        raw_savs.wait_recv()
        raw_grads.wait_recv()
        backs.wait_recv()
        came = back_in[...].astype(F32)
        far_tilt = jnp.sum(jnp.where((lane == rank) | (lane == rank + 1), came, 0.0), axis=1, keepdims=True)
        far_keep = jnp.sum(jnp.where(lane == rank + 2, came, 0.0), axis=1, keepdims=True)
        far_back = came[:, :rank].astype(BF16)
        for a in range(0, raw_b, chunk):
            b = min(a + chunk, raw_b)
            cols = slice(width - raw_b + a, width - raw_b + b)
            normed = jnp.dot(far_back, raw_down[:, a:b], preferred_element_type=F32)
            next_gr[:, cols] = (
                jnp.where(far_keep > 0.5, raw_grad[:, a:b].astype(F32), 0.0)
                + raw_gain[:, cols].astype(F32) * normed
                - raw_sav[:, a:b].astype(F32) * far_tilt
            ).astype(BF16)

    @pl.when(sec < n_sec - 1)
    def _():
        for copy in up_way:
            copy.wait_send()
        for c in range(len(done_f)):
            shift(0, out_f, next_in, c).wait_send()
        for c in range(len(done_b)):
            shift(1, out_b, next_gr, c).wait_recv()

    @pl.when(sec > 0)
    def _():
        for copy in down_way:
            copy.wait_send()
        for c in range(len(done_b)):
            shift(1, out_b, next_gr, c).wait_send()
        for c in range(len(done_f)):
            shift(0, out_f, next_in, c).wait_recv()


def place(*refs):
    count = len(refs) // 2
    sems = refs[-1]
    copies = [pltpu.make_async_copy(refs[i], refs[count + i], sems.at[i]) for i in range(count)]
    for copy in copies:
        copy.start()
    for copy in copies:
        copy.wait()


def solution(mesh):
    n_sec, n_ten, n_dp = (mesh.shape[name] for name in ("section", "tensor", "dp"))

    def shards(forward_rows, saved_rows, output_grad, lengths, norm_gain, down_map, up_map):
        rows, width = forward_rows.shape[2:]
        rank = down_map.shape[1]
        share = rank // n_dp
        bits = n_ten.bit_length() - 1
        chunk = min(width, 4 * LANES)
        n_chunk = width // chunk
        raw_f = int(width * RAW_FORWARD) // LANES * LANES
        raw_b = int(width * RAW_BACK) // LANES * LANES
        wide = -(-(rank + 4) // LANES) * LANES
        steps = max(bits, 1)
        vmem = pl.BlockSpec(memory_space=pltpu.VMEM)
        anywhere = pl.BlockSpec(memory_space=pl.ANY)
        flops = 7 * 2 * rows * rank * width
        dma = pltpu.SemaphoreType.DMA
        shapes = ((rows, width),) * 2 + ((share, width),) * 2
        results = pl.pallas_call(
            functools.partial(tick, (n_sec, n_ten, n_dp, chunk)),
            out_shape=tuple(pltpu.VMEM(shape, BF16) for shape in shapes),
            in_specs=[anywhere, anywhere, anywhere, pl.BlockSpec(memory_space=pltpu.SMEM), vmem, anywhere, anywhere],
            out_specs=(vmem,) * 4,
            scratch_shapes=[
                pltpu.VMEM((rows, width), BF16),
                pltpu.VMEM((rows, width), BF16),
                pltpu.VMEM((rows, width), BF16),
                pltpu.VMEM((rank, width), BF16),
                pltpu.VMEM((rank, width), BF16),
                pltpu.VMEM((rows, width), BF16),
                pltpu.VMEM((rows, wide), F32),
                pltpu.VMEM((rows, 2 * rank), F32),
                pltpu.VMEM((steps, rows, wide), BF16),
                pltpu.VMEM((steps, rows, wide), BF16),
                pltpu.VMEM((steps, rows, 2 * rank), BF16),
                pltpu.VMEM((steps, rows, 2 * rank), BF16),
                pltpu.VMEM((rows, width), BF16),
                pltpu.VMEM((rows, width), BF16),
                pltpu.VMEM((2, rank, width), BF16),
                pltpu.VMEM((2, max(n_dp - 1, 1), share, width), BF16),
                pltpu.VMEM((rows // 2, 2 * rank), BF16),
                pltpu.VMEM((rows // 2, 2 * rank), BF16),
                pltpu.VMEM((rows, wide), BF16),
                pltpu.VMEM((rows, wide), BF16),
                pltpu.VMEM((rows, raw_f), BF16),
                pltpu.VMEM((rank, raw_f), BF16),
                pltpu.VMEM((rows, raw_b), BF16),
                pltpu.VMEM((rows, raw_b), BF16),
                pltpu.VMEM((rank, raw_b), BF16),
                pltpu.VMEM((1, width), BF16),
                dma((5,)),
                dma((2, steps)),
                dma((2, steps)),
                dma((2, steps)),
                dma((2, steps)),
                dma((2, n_chunk)),
                dma((2, n_chunk)),
                dma((2, max(n_dp - 1, 1))),
                dma((2, max(n_dp - 1, 1))),
                dma((8,)),
                dma((8,)),
                dma((2, max(n_dp - 1, 1))),
                dma((2, max(n_dp - 1, 1))),
            ],
            compiler_params=pltpu.CompilerParams(collective_id=0, has_side_effects=True),
            cost_estimate=pl.CostEstimate(
                flops=flops, bytes_accessed=16 * rows * width, transcendentals=4 * rows * rank
            ),
            name="tick",
        )(
            forward_rows[0, 0], saved_rows[0, 0], output_grad[0, 0], lengths[0], norm_gain, down_map[0], up_map[0]
        )
        next_inputs, next_grads, grad_down, grad_up = pl.pallas_call(
            place,
            out_shape=tuple(jax.ShapeDtypeStruct(shape, BF16) for shape in shapes),
            in_specs=[vmem] * 4,
            out_specs=(anywhere,) * 4,
            scratch_shapes=[dma((4,))],
            name="place",
        )(*[pltpu.with_memory_space_constraint(x, pltpu.VMEM) for x in results])
        return next_inputs[None, None], next_grads[None, None], grad_down[None], grad_up[None]

    row_spec = P("section", "dp", None, "tensor")
    map_spec = P("section", None, "tensor")
    part_spec = P("section", "dp", "tensor")
    return jax.shard_map(
        shards,
        mesh=mesh,
        in_specs=(row_spec, row_spec, row_spec, P("section", "dp"), P("section", "tensor"), map_spec, map_spec),
        out_specs=(row_spec, row_spec, part_spec, part_spec),
        check_vma=False,
    )
```

```python
import functools

import jax
import jax.numpy as jnp
from jax import lax
from jax.experimental import pallas as pl
from jax.experimental.pallas import tpu as pltpu
from jax.sharding import PartitionSpec as P

EPSILON = 1e-05
LANES = 128
RAW_FORWARD = 0.375
RAW_BACK = 0.125
BLOCKS = 4
F32 = jnp.float32
BF16 = jnp.bfloat16


def contract_last(left_side, right_side):
    return lax.dot_general(
        left_side, right_side, (((1,), (1,)), ((), ())), preferred_element_type=F32
    )


def contract_rows(left_side, right_side):
    return lax.dot_general(
        left_side, right_side, (((0,), (0,)), ((), ())), preferred_element_type=F32
    )


def flip(index, bit):
    step = 1 << bit
    return index + step * (1 - 2 * ((index // step) % 2))


def tick(sizes, fwd_hbm, sav_hbm, grad_hbm, len_ref, gain_ref, down_hbm, up_hbm,
         next_in, next_gr, grad_down, grad_up,
         fwd, sav, kept, down, up, scaled,
         acc_f, acc_b, send_f, recv_f, send_b, recv_b, out_f, out_b,
         part, part_recv, act_out, act_in, back_out, back_in,
         side_out, side_in, sq_out, sq_in, sq_send_sem, sq_recv_sem,
         raw_fwd, raw_up, raw_sav, raw_grad, raw_down, raw_gain, load_sem,
         f_send_sem, f_recv_sem, b_send_sem, b_recv_sem,
         sec_send_sem, sec_recv_sem, dp_send_sem, dp_recv_sem,
         raw_send_sem, raw_recv_sem, relay_send_sem, relay_recv_sem):
    n_sec, n_ten, n_dp, chunk = sizes
    rows, width = fwd.shape
    rank = down.shape[0]
    full_width = width * n_ten
    n_seq = len_ref.shape[1]
    bits = n_ten.bit_length() - 1
    half = rows // 2
    n_chunk = width // chunk
    share = rank // n_dp
    sec, ten, dp = lax.axis_index("section"), lax.axis_index("tensor"), lax.axis_index("dp")

    loads = [
        pltpu.make_async_copy(src, dst, load_sem.at[i])
        for i, (src, dst) in enumerate(
            ((fwd_hbm, fwd), (down_hbm, down), (sav_hbm, sav), (grad_hbm, kept), (up_hbm, up))
        )
    ]
    for i in (2, 1, 3, 4, 0):
        loads[i].start()

    barrier = pltpu.get_barrier_semaphore()
    for k in range(1, n_ten):
        pl.semaphore_signal(barrier, inc=1, device_id={"tensor": (ten + k) % n_ten})
    for k in range(1, n_dp):
        pl.semaphore_signal(barrier, inc=1, device_id={"dp": (dp + k) % n_dp})

    @pl.when(sec > 0)
    def _():
        pl.semaphore_signal(barrier, inc=1, device_id={"section": sec - 1})

    @pl.when(sec < n_sec - 1)
    def _():
        pl.semaphore_signal(barrier, inc=1, device_id={"section": sec + 1})

    columns = [slice(c * chunk, (c + 1) * chunk) for c in range(n_chunk)]
    raw_f, raw_b = raw_fwd.shape[1], raw_sav.shape[1]
    mine = pl.ds(pl.multiple_of(dp * share, share), share)
    tail_f, tail_b = pl.ds(width - raw_f, raw_f), pl.ds(width - raw_b, raw_b)

    def across(i, source, target, step):
        return pltpu.make_async_remote_copy(
            src_ref=source,
            dst_ref=target,
            send_sem=raw_send_sem.at[i],
            recv_sem=raw_recv_sem.at[i],
            device_id={"section": sec + step},
        )

    raw_ups = across(0, up_hbm.at[mine, tail_f], raw_up.at[mine], 1)
    raw_fwds = across(1, fwd_hbm.at[:, tail_f], raw_fwd, 1)
    acts = across(2, act_out, act_in, 1)
    raw_downs = across(3, down_hbm.at[mine, tail_b], raw_down.at[mine], -1)
    raw_gains = across(4, gain_ref, raw_gain, -1)
    raw_savs = across(5, sav_hbm.at[:, tail_b], raw_sav, -1)
    raw_grads = across(6, grad_hbm.at[:, tail_b], raw_grad, -1)
    backs = across(7, back_out, back_in, -1)
    sides = across(8, side_out, side_in, -1)
    up_way, down_way = (raw_ups, raw_fwds, acts), (raw_downs, raw_gains, raw_savs, raw_grads, backs, sides)

    def relay(way, k):
        ref = (raw_up, raw_down)[way].at[mine]
        return pltpu.make_async_remote_copy(
            src_ref=ref,
            dst_ref=ref,
            send_sem=relay_send_sem.at[way, k - 1],
            recv_sem=relay_recv_sem.at[way, k - 1],
            device_id={"dp": (dp + k) % n_dp},
        )

    pl.semaphore_wait(barrier, n_ten - 1 + n_dp - 1 + jnp.where(sec > 0, 1, 0) + jnp.where(sec < n_sec - 1, 1, 0))

    @pl.when(sec < n_sec - 1)
    def _():
        for copy in up_way[:-1]:
            copy.start()

    @pl.when(sec > 0)
    def _():
        for copy in down_way[:-2]:
            copy.start()

    def exchange(form, q, p):
        acc, send, recv, send_sem, recv_sem, blocks = form
        span = pl.ds(q * (rows // blocks), rows // blocks)
        return pltpu.make_async_remote_copy(
            src_ref=send.at[p, span],
            dst_ref=recv.at[p, span],
            send_sem=send_sem.at[q, p],
            recv_sem=recv_sem.at[q, p],
            device_id={"tensor": flip(ten, (q + p) % bits)},
        )

    form_f = (acc_f, send_f, recv_f, f_send_sem, f_recv_sem, 2)
    form_b = (acc_b, send_b, recv_b, b_send_sem, b_recv_sem, BLOCKS)

    def begin(form, q, p):
        acc, send, blocks = form[0], form[1], form[5]
        span = pl.ds(q * (rows // blocks), rows // blocks)
        send[p, span] = acc[span].astype(BF16)
        exchange(form, q, p).start()

    def finish(form, q, p):
        acc, recv, blocks = form[0], form[2], form[5]
        span = pl.ds(q * (rows // blocks), rows // blocks)
        exchange(form, q, p).wait()
        acc[span] = acc[span] + recv[p, span].astype(F32)

    eye = lax.broadcasted_iota(jnp.int32, (rows, rows), 0) == lax.broadcasted_iota(jnp.int32, (rows, rows), 1)

    def to_row(column):
        return jnp.sum(jnp.where(eye, column, 0.0), axis=0, keepdims=True)

    def to_column(row):
        return jnp.sum(jnp.where(eye, row, 0.0), axis=1, keepdims=True)

    def squares(i, k):
        return pltpu.make_async_remote_copy(
            src_ref=sq_out.at[i],
            dst_ref=sq_in.at[i, k - 1],
            send_sem=sq_send_sem.at[i, k - 1],
            recv_sem=sq_recv_sem.at[i, k - 1],
            device_id={"tensor": (ten + k) % n_ten},
        )

    def spread(i, column):
        sq_out[i] = jnp.broadcast_to(to_row(column), (8, rows))
        for k in range(1, n_ten):
            squares(i, k).start()

    def scale_of(i):
        row = sq_out[i, 0:1]
        for k in range(1, n_ten):
            squares(i, k).wait()
            row += sq_in[i, k - 1, 0:1]
        return lax.rsqrt(to_column(row) / full_width + EPSILON)

    load_fwd, load_down, load_sav, load_grad, load_up = loads
    load_sav.wait()
    square_s = jnp.zeros((rows, 1), F32)
    for cols in columns:
        values = sav[:, cols].astype(F32)
        square_s += jnp.sum(values * values, axis=1, keepdims=True)
        scaled[:, cols] = (values * gain_ref[:, cols].astype(F32)).astype(BF16)
    spread(0, square_s)
    load_down.wait()
    total_s = jnp.zeros((rows, rank), F32)
    for cols in columns:
        total_s += contract_last(scaled[:, cols], down[:, cols])
    load_grad.wait()
    load_up.wait()
    position = lax.broadcasted_iota(jnp.int32, (rows, 1), 0)
    seq_rows = rows // n_seq
    limit = jnp.full((rows, 1), 0, jnp.int32)
    for i in range(n_seq):
        limit = jnp.where(position >= i * seq_rows, i * seq_rows + len_ref[0, i], limit)
    keep = position < limit
    total_g = jnp.zeros((rows, rank), F32)
    for cols in columns:
        held = jnp.where(keep, kept[:, cols].astype(F32), 0.0).astype(BF16)
        kept[:, cols] = held
        total_g += contract_last(held, up[:, cols])
    acc_b[...] = jnp.concatenate([total_g, total_s], axis=1)
    if bits:
        for q in range(BLOCKS):
            begin(form_b, q, 0)

    load_fwd.wait()
    total = jnp.zeros((rows, rank), F32)
    square_f = jnp.zeros((rows, 1), F32)
    for cols in columns:
        values = fwd[:, cols].astype(F32)
        square_f += jnp.sum(values * values, axis=1, keepdims=True)
        gained = (values * gain_ref[:, cols].astype(F32)).astype(BF16)
        total += contract_last(gained, down[:, cols])
    acc_f[...] = total
    spread(1, square_f)
    if bits:
        for q in range(2):
            begin(form_f, q, 0)
    for p in range(1, bits):
        for q in range(BLOCKS):
            finish(form_b, q, p - 1)
            begin(form_b, q, p)
        for q in range(2):
            finish(form_f, q, p - 1)
            begin(form_f, q, p)

    done_f = [slice(a, min(a + chunk, width - raw_f)) for a in range(0, width - raw_f, chunk)]
    done_b = [slice(a, min(a + chunk, width - raw_b)) for a in range(0, width - raw_b, chunk)]

    def shift(way, source, target, g, c):
        cols = (done_f, done_b)[way][c]
        span = pl.ds(cols.start, cols.stop - cols.start)
        part_rows = pl.ds(g * half, half)
        return pltpu.make_async_remote_copy(
            src_ref=source.at[part_rows, span],
            dst_ref=target.at[part_rows, span],
            send_sem=sec_send_sem.at[way, g, c],
            recv_sem=sec_recv_sem.at[way, g, c],
            device_id={"section": sec + 1 if way == 0 else sec - 1},
        )

    def shifts(way):
        source, target = ((out_f, next_in), (out_b, next_gr))[way]
        return [shift(way, source, target, g, c) for g in range(2) for c in range(len((done_f, done_b)[way]))]

    scale_s = scale_of(0)
    acts_s, backs_s, tilts = [], [], []
    for g in range(2):
        span = slice(g * half, (g + 1) * half)
        if bits:
            for q in range(g * BLOCKS // 2, (g + 1) * BLOCKS // 2):
                finish(form_b, q, bits - 1)
        own_scale = scale_s[span]
        slope = acc_b[span, :rank]
        rank_s = acc_b[span, rank:] * own_scale
        gate = jax.nn.sigmoid(rank_s)
        acts_s.append((rank_s * gate).astype(BF16))
        back = slope * (gate * (1.0 + rank_s * (1.0 - gate)))
        tilt = jnp.sum(back.astype(BF16).astype(F32) * rank_s, axis=1, keepdims=True) * (own_scale * own_scale / full_width)
        back_s = back * own_scale
        back_rows = back_s.astype(BF16)
        backs_s.append(back_s)
        tilts.append(tilt)

        @pl.when(sec > 0)
        def _():
            if g == 1:
                back_out[...] = jnp.concatenate(backs_s, axis=1).astype(BF16)
                top = lax.broadcasted_iota(jnp.int32, (8, rows), 0) == 0
                side_out[...] = jnp.where(
                    top, to_row(jnp.concatenate(tilts, axis=0)), to_row(jnp.where(keep, 1.0, 0.0))
                )
                backs.start()
                sides.start()
            for c, cols in enumerate(done_b):
                normed = jnp.dot(back_rows, down[:, cols], preferred_element_type=F32)
                out_b[span, cols] = (
                    kept[span, cols].astype(F32)
                    + gain_ref[:, cols].astype(F32) * normed
                    - sav[span, cols].astype(F32) * tilt
                ).astype(BF16)
                shift(1, out_b, next_gr, g, c).start()

    back_scaled = jnp.concatenate(backs_s, axis=0).astype(BF16)
    act_s = jnp.concatenate(acts_s, axis=0)

    scale_f = scale_of(1)
    if bits:
        for q in range(2):
            finish(form_f, q, bits - 1)
    rank_f = acc_f[...] * scale_f
    act_f = rank_f * jax.nn.sigmoid(rank_f)

    @pl.when(sec < n_sec - 1)
    def _():
        act_out[...] = jnp.concatenate([act_f[:half], act_f[half:]], axis=1).astype(BF16)
        acts.start()

    act_f = act_f.astype(BF16)

    @pl.when(sec < n_sec - 1)
    def _():
        for c, cols in enumerate(done_f):
            grown = jnp.dot(act_f, up[:, cols], preferred_element_type=F32)
            out_f[:, cols] = (fwd[:, cols].astype(F32) + grown).astype(BF16)
            for g in range(2):
                shift(0, out_f, next_in, g, c).start()

    def trade(i, k):
        target = (dp + k) % n_dp
        return pltpu.make_async_remote_copy(
            src_ref=part.at[i, pl.ds(pl.multiple_of(target * share, share), share)],
            dst_ref=part_recv.at[i, k - 1],
            send_sem=dp_send_sem.at[i, k - 1],
            recv_sem=dp_recv_sem.at[i, k - 1],
            device_id={"dp": target},
        )

    for i, (left_side, right_side) in enumerate(((back_scaled, scaled), (act_s, kept))):
        for cols in columns:
            part[i, :, cols] = contract_rows(left_side, right_side[:, cols]).astype(BF16)
        for k in range(1, n_dp):
            trade(i, k).start()

    @pl.when(sec > 0)
    def _():
        raw_ups.wait_recv()
        for k in range(1, n_dp):
            relay(0, k).start()

    @pl.when(sec < n_sec - 1)
    def _():
        raw_downs.wait_recv()
        for k in range(1, n_dp):
            relay(1, k).start()

    for i, out in enumerate((grad_down, grad_up)):
        for k in range(1, n_dp):
            trade(i, k).wait()
        for cols in columns:
            summed = part[i, mine, cols].astype(F32)
            for k in range(1, n_dp):
                summed += part_recv[i, k - 1, :, cols].astype(F32)
            out[:, cols] = (summed * (1.0 / n_dp)).astype(BF16)

    @pl.when(sec == 0)
    def _():
        next_in[...] = jnp.zeros_like(next_in)

    @pl.when(sec == n_sec - 1)
    def _():
        next_gr[...] = jnp.zeros_like(next_gr)

    @pl.when(sec > 0)
    def _():
        for k in range(1, n_dp):
            relay(0, k).wait()
        raw_fwds.wait_recv()
        acts.wait_recv()
        came = act_in[...].astype(F32)
        came = jnp.concatenate([came[:, :rank], came[:, rank:]], axis=0).astype(BF16)
        for a in range(0, raw_f, chunk):
            b = min(a + chunk, raw_f)
            grown = jnp.dot(came, raw_up[:, a:b], preferred_element_type=F32)
            next_in[:, width - raw_f + a:width - raw_f + b] = (raw_fwd[:, a:b].astype(F32) + grown).astype(BF16)

    @pl.when(sec < n_sec - 1)
    def _():
        for k in range(1, n_dp):
            relay(1, k).wait()
        raw_gains.wait_recv()
        raw_savs.wait_recv()
        raw_grads.wait_recv()
        backs.wait_recv()
        sides.wait_recv()
        came = back_in[...].astype(F32)
        far_back = jnp.concatenate([came[:, :rank], came[:, rank:]], axis=0).astype(BF16)
        far_tilt = to_column(side_in[0:1])
        far_keep = to_column(side_in[1:2])
        for a in range(0, raw_b, chunk):
            b = min(a + chunk, raw_b)
            cols = slice(width - raw_b + a, width - raw_b + b)
            normed = jnp.dot(far_back, raw_down[:, a:b], preferred_element_type=F32)
            next_gr[:, cols] = (
                jnp.where(far_keep > 0.5, raw_grad[:, a:b].astype(F32), 0.0)
                + raw_gain[:, cols].astype(F32) * normed
                - raw_sav[:, a:b].astype(F32) * far_tilt
            ).astype(BF16)

    @pl.when(sec < n_sec - 1)
    def _():
        for copy in up_way:
            copy.wait_send()
        for copy in shifts(0):
            copy.wait_send()
        for copy in shifts(1):
            copy.wait_recv()

    @pl.when(sec > 0)
    def _():
        for copy in down_way:
            copy.wait_send()
        for copy in shifts(1):
            copy.wait_send()
        for copy in shifts(0):
            copy.wait_recv()


def place(*refs):
    count = len(refs) // 2
    sems = refs[-1]
    copies = [pltpu.make_async_copy(refs[i], refs[count + i], sems.at[i]) for i in range(count)]
    for copy in copies:
        copy.start()
    for copy in copies:
        copy.wait()


def solution(mesh):
    n_sec, n_ten, n_dp = (mesh.shape[name] for name in ("section", "tensor", "dp"))

    def shards(forward_rows, saved_rows, output_grad, lengths, norm_gain, down_map, up_map):
        rows, width = forward_rows.shape[2:]
        rank = down_map.shape[1]
        share = rank // n_dp
        bits = n_ten.bit_length() - 1
        chunk = min(width, 4 * LANES)
        n_chunk = width // chunk
        raw_f = int(width * RAW_FORWARD) // LANES * LANES
        raw_b = int(width * RAW_BACK) // LANES * LANES
        peers = max(n_ten - 1, 1)
        steps = max(bits, 1)
        vmem = pl.BlockSpec(memory_space=pltpu.VMEM)
        anywhere = pl.BlockSpec(memory_space=pl.ANY)
        flops = 7 * 2 * rows * rank * width
        dma = pltpu.SemaphoreType.DMA
        shapes = ((rows, width),) * 2 + ((share, width),) * 2
        results = pl.pallas_call(
            functools.partial(tick, (n_sec, n_ten, n_dp, chunk)),
            out_shape=tuple(pltpu.VMEM(shape, BF16) for shape in shapes),
            in_specs=[anywhere, anywhere, anywhere, pl.BlockSpec(memory_space=pltpu.SMEM), vmem, anywhere, anywhere],
            out_specs=(vmem,) * 4,
            scratch_shapes=[
                pltpu.VMEM((rows, width), BF16),
                pltpu.VMEM((rows, width), BF16),
                pltpu.VMEM((rows, width), BF16),
                pltpu.VMEM((rank, width), BF16),
                pltpu.VMEM((rank, width), BF16),
                pltpu.VMEM((rows, width), BF16),
                pltpu.VMEM((rows, rank), F32),
                pltpu.VMEM((rows, 2 * rank), F32),
                pltpu.VMEM((steps, rows, rank), BF16),
                pltpu.VMEM((steps, rows, rank), BF16),
                pltpu.VMEM((steps, rows, 2 * rank), BF16),
                pltpu.VMEM((steps, rows, 2 * rank), BF16),
                pltpu.VMEM((rows, width), BF16),
                pltpu.VMEM((rows, width), BF16),
                pltpu.VMEM((2, rank, width), BF16),
                pltpu.VMEM((2, max(n_dp - 1, 1), share, width), BF16),
                pltpu.VMEM((rows // 2, 2 * rank), BF16),
                pltpu.VMEM((rows // 2, 2 * rank), BF16),
                pltpu.VMEM((rows // 2, 2 * rank), BF16),
                pltpu.VMEM((rows // 2, 2 * rank), BF16),
                pltpu.VMEM((8, rows), F32),
                pltpu.VMEM((8, rows), F32),
                pltpu.VMEM((2, 8, rows), F32),
                pltpu.VMEM((2, peers, 8, rows), F32),
                dma((2, peers)),
                dma((2, peers)),
                pltpu.VMEM((rows, raw_f), BF16),
                pltpu.VMEM((rank, raw_f), BF16),
                pltpu.VMEM((rows, raw_b), BF16),
                pltpu.VMEM((rows, raw_b), BF16),
                pltpu.VMEM((rank, raw_b), BF16),
                pltpu.VMEM((1, width), BF16),
                dma((5,)),
                dma((2, steps)),
                dma((2, steps)),
                dma((BLOCKS, steps)),
                dma((BLOCKS, steps)),
                dma((2, 2, n_chunk)),
                dma((2, 2, n_chunk)),
                dma((2, max(n_dp - 1, 1))),
                dma((2, max(n_dp - 1, 1))),
                dma((9,)),
                dma((9,)),
                dma((2, max(n_dp - 1, 1))),
                dma((2, max(n_dp - 1, 1))),
            ],
            compiler_params=pltpu.CompilerParams(collective_id=0, has_side_effects=True),
            cost_estimate=pl.CostEstimate(
                flops=flops, bytes_accessed=16 * rows * width, transcendentals=4 * rows * rank
            ),
            name="tick",
        )(
            forward_rows[0, 0], saved_rows[0, 0], output_grad[0, 0], lengths[0], norm_gain, down_map[0], up_map[0]
        )
        next_inputs, next_grads, grad_down, grad_up = pl.pallas_call(
            place,
            out_shape=tuple(jax.ShapeDtypeStruct(shape, BF16) for shape in shapes),
            in_specs=[vmem] * 4,
            out_specs=(anywhere,) * 4,
            scratch_shapes=[dma((4,))],
            name="place",
        )(*[pltpu.with_memory_space_constraint(x, pltpu.VMEM) for x in results])
        return next_inputs[None, None], next_grads[None, None], grad_down[None], grad_up[None]

    row_spec = P("section", "dp", None, "tensor")
    map_spec = P("section", None, "tensor")
    part_spec = P("section", "dp", "tensor")
    return jax.shard_map(
        shards,
        mesh=mesh,
        in_specs=(row_spec, row_spec, row_spec, P("section", "dp"), P("section", "tensor"), map_spec, map_spec),
        out_specs=(row_spec, row_spec, part_spec, part_spec),
        check_vma=False,
    )
```

```python
import functools

import jax
import jax.numpy as jnp
from jax import lax
from jax.experimental import pallas as pl
from jax.experimental.pallas import tpu as pltpu
from jax.sharding import PartitionSpec as P

EPSILON = 1e-05
LANES = 128
RAW_FORWARD = 0.4375
RAW_BACK = 0.1875
BLOCKS = 4
F32 = jnp.float32
BF16 = jnp.bfloat16


def contract_last(left_side, right_side):
    return lax.dot_general(
        left_side, right_side, (((1,), (1,)), ((), ())), preferred_element_type=F32
    )


def contract_rows(left_side, right_side):
    return lax.dot_general(
        left_side, right_side, (((0,), (0,)), ((), ())), preferred_element_type=F32
    )


def flip(index, bit):
    step = 1 << bit
    return index + step * (1 - 2 * ((index // step) % 2))


def tick(sizes, fwd_hbm, sav_hbm, grad_hbm, len_ref, gain_ref, down_hbm, up_hbm,
         next_in, next_gr, grad_down, grad_up,
         fwd, sav, kept, down, up, scaled,
         acc_f, acc_b, send_f, recv_f, send_b, recv_b, out_f, out_b,
         part, part_recv, act_out, act_in, back_out, back_in,
         side_out, side_in, sq_out, sq_in, sq_send_sem, sq_recv_sem,
         raw_fwd, raw_up, raw_sav, raw_grad, raw_down, raw_gain, load_sem,
         f_send_sem, f_recv_sem, b_send_sem, b_recv_sem,
         sec_send_sem, sec_recv_sem, dp_send_sem, dp_recv_sem,
         raw_send_sem, raw_recv_sem, relay_send_sem, relay_recv_sem):
    n_sec, n_ten, n_dp, chunk = sizes
    rows, width = fwd.shape
    rank = down.shape[0]
    full_width = width * n_ten
    n_seq = len_ref.shape[1]
    bits = n_ten.bit_length() - 1
    half = rows // 2
    n_chunk = width // chunk
    share = rank // n_dp
    sec, ten, dp = lax.axis_index("section"), lax.axis_index("tensor"), lax.axis_index("dp")

    loads = [
        pltpu.make_async_copy(src, dst, load_sem.at[i])
        for i, (src, dst) in enumerate(
            ((fwd_hbm, fwd), (down_hbm, down), (sav_hbm, sav), (grad_hbm, kept), (up_hbm, up))
        )
    ]
    for i in (2, 1, 3, 4, 0):
        loads[i].start()

    barrier = pltpu.get_barrier_semaphore()
    for k in range(1, n_ten):
        pl.semaphore_signal(barrier, inc=1, device_id={"tensor": (ten + k) % n_ten})
    for k in range(1, n_dp):
        pl.semaphore_signal(barrier, inc=1, device_id={"dp": (dp + k) % n_dp})

    @pl.when(sec > 0)
    def _():
        pl.semaphore_signal(barrier, inc=1, device_id={"section": sec - 1})

    @pl.when(sec < n_sec - 1)
    def _():
        pl.semaphore_signal(barrier, inc=1, device_id={"section": sec + 1})

    columns = [slice(c * chunk, (c + 1) * chunk) for c in range(n_chunk)]
    raw_f, raw_b = raw_fwd.shape[1], raw_sav.shape[1]
    mine = pl.ds(pl.multiple_of(dp * share, share), share)
    tail_f, tail_b = pl.ds(width - raw_f, raw_f), pl.ds(width - raw_b, raw_b)

    def across(i, source, target, step):
        return pltpu.make_async_remote_copy(
            src_ref=source,
            dst_ref=target,
            send_sem=raw_send_sem.at[i],
            recv_sem=raw_recv_sem.at[i],
            device_id={"section": sec + step},
        )

    raw_ups = across(0, up_hbm.at[mine, tail_f], raw_up.at[mine], 1)
    raw_fwds = across(1, fwd_hbm.at[:, tail_f], raw_fwd, 1)
    acts = across(2, act_out, act_in, 1)
    raw_downs = across(3, down_hbm.at[mine, tail_b], raw_down.at[mine], -1)
    raw_gains = across(4, gain_ref, raw_gain, -1)
    raw_savs = across(5, sav_hbm.at[:, tail_b], raw_sav, -1)
    raw_grads = across(6, grad_hbm.at[:, tail_b], raw_grad, -1)
    backs = across(7, back_out, back_in, -1)
    sides = across(8, side_out, side_in, -1)
    up_way, down_way = (raw_ups, raw_fwds, acts), (raw_downs, raw_gains, raw_savs, raw_grads, backs, sides)

    def relay(way, k):
        ref = (raw_up, raw_down)[way].at[mine]
        return pltpu.make_async_remote_copy(
            src_ref=ref,
            dst_ref=ref,
            send_sem=relay_send_sem.at[way, k - 1],
            recv_sem=relay_recv_sem.at[way, k - 1],
            device_id={"dp": (dp + k) % n_dp},
        )

    pl.semaphore_wait(barrier, n_ten - 1 + n_dp - 1 + jnp.where(sec > 0, 1, 0) + jnp.where(sec < n_sec - 1, 1, 0))

    @pl.when(sec < n_sec - 1)
    def _():
        for copy in up_way[:-1]:
            copy.start()

    @pl.when(sec > 0)
    def _():
        for copy in down_way[:-2]:
            copy.start()

    def exchange(form, q, p):
        acc, send, recv, send_sem, recv_sem, blocks = form
        span = pl.ds(q * (rows // blocks), rows // blocks)
        return pltpu.make_async_remote_copy(
            src_ref=send.at[p, span],
            dst_ref=recv.at[p, span],
            send_sem=send_sem.at[q, p],
            recv_sem=recv_sem.at[q, p],
            device_id={"tensor": flip(ten, (q + p) % bits)},
        )

    form_f = (acc_f, send_f, recv_f, f_send_sem, f_recv_sem, 2)
    form_b = (acc_b, send_b, recv_b, b_send_sem, b_recv_sem, BLOCKS)

    def begin(form, q, p):
        acc, send, blocks = form[0], form[1], form[5]
        span = pl.ds(q * (rows // blocks), rows // blocks)
        send[p, span] = acc[span].astype(BF16)
        exchange(form, q, p).start()

    def finish(form, q, p):
        acc, recv, blocks = form[0], form[2], form[5]
        span = pl.ds(q * (rows // blocks), rows // blocks)
        exchange(form, q, p).wait()
        acc[span] = acc[span] + recv[p, span].astype(F32)

    eye = lax.broadcasted_iota(jnp.int32, (rows, rows), 0) == lax.broadcasted_iota(jnp.int32, (rows, rows), 1)

    def to_row(column):
        return jnp.sum(jnp.where(eye, column, 0.0), axis=0, keepdims=True)

    def to_column(row):
        return jnp.sum(jnp.where(eye, row, 0.0), axis=1, keepdims=True)

    def squares(i, k):
        return pltpu.make_async_remote_copy(
            src_ref=sq_out.at[i],
            dst_ref=sq_in.at[i, k - 1],
            send_sem=sq_send_sem.at[i, k - 1],
            recv_sem=sq_recv_sem.at[i, k - 1],
            device_id={"tensor": (ten + k) % n_ten},
        )

    def spread(i, column):
        sq_out[i] = jnp.broadcast_to(to_row(column), (8, rows))
        for k in range(1, n_ten):
            squares(i, k).start()

    def scale_of(i):
        row = sq_out[i, 0:1]
        for k in range(1, n_ten):
            squares(i, k).wait()
            row += sq_in[i, k - 1, 0:1]
        return lax.rsqrt(to_column(row) / full_width + EPSILON)

    load_fwd, load_down, load_sav, load_grad, load_up = loads
    load_sav.wait()
    square_s = jnp.zeros((rows, 1), F32)
    for cols in columns:
        values = sav[:, cols].astype(F32)
        square_s += jnp.sum(values * values, axis=1, keepdims=True)
        scaled[:, cols] = (values * gain_ref[:, cols].astype(F32)).astype(BF16)
    spread(0, square_s)
    load_down.wait()
    total_s = jnp.zeros((rows, rank), F32)
    for cols in columns:
        total_s += contract_last(scaled[:, cols], down[:, cols])
    load_grad.wait()
    load_up.wait()
    position = lax.broadcasted_iota(jnp.int32, (rows, 1), 0)
    seq_rows = rows // n_seq
    limit = jnp.full((rows, 1), 0, jnp.int32)
    for i in range(n_seq):
        limit = jnp.where(position >= i * seq_rows, i * seq_rows + len_ref[0, i], limit)
    keep = position < limit
    total_g = jnp.zeros((rows, rank), F32)
    for cols in columns:
        held = jnp.where(keep, kept[:, cols].astype(F32), 0.0).astype(BF16)
        kept[:, cols] = held
        total_g += contract_last(held, up[:, cols])
    acc_b[...] = jnp.concatenate([total_g, total_s], axis=1)
    if bits:
        for q in range(BLOCKS):
            begin(form_b, q, 0)

    load_fwd.wait()
    total = jnp.zeros((rows, rank), F32)
    square_f = jnp.zeros((rows, 1), F32)
    for cols in columns:
        values = fwd[:, cols].astype(F32)
        square_f += jnp.sum(values * values, axis=1, keepdims=True)
        gained = (values * gain_ref[:, cols].astype(F32)).astype(BF16)
        total += contract_last(gained, down[:, cols])
    acc_f[...] = total
    spread(1, square_f)
    if bits:
        for q in range(2):
            begin(form_f, q, 0)
    for p in range(1, bits):
        for q in range(BLOCKS):
            finish(form_b, q, p - 1)
            begin(form_b, q, p)
        for q in range(2):
            finish(form_f, q, p - 1)
            begin(form_f, q, p)

    done_f = [slice(a, min(a + chunk, width - raw_f)) for a in range(0, width - raw_f, chunk)]
    done_b = [slice(a, min(a + chunk, width - raw_b)) for a in range(0, width - raw_b, chunk)]

    def shift(way, source, target, g, c):
        cols = (done_f, done_b)[way][c]
        span = pl.ds(cols.start, cols.stop - cols.start)
        part_rows = pl.ds(g * half, half)
        return pltpu.make_async_remote_copy(
            src_ref=source.at[part_rows, span],
            dst_ref=target.at[part_rows, span],
            send_sem=sec_send_sem.at[way, g, c],
            recv_sem=sec_recv_sem.at[way, g, c],
            device_id={"section": sec + 1 if way == 0 else sec - 1},
        )

    def shifts(way):
        source, target = ((out_f, next_in), (out_b, next_gr))[way]
        return [shift(way, source, target, g, c) for g in range(2) for c in range(len((done_f, done_b)[way]))]

    scale_s = scale_of(0)
    acts_s, backs_s, tilts = [], [], []
    for g in range(2):
        span = slice(g * half, (g + 1) * half)
        if bits:
            for q in range(g * BLOCKS // 2, (g + 1) * BLOCKS // 2):
                finish(form_b, q, bits - 1)
        own_scale = scale_s[span]
        slope = acc_b[span, :rank]
        rank_s = acc_b[span, rank:] * own_scale
        gate = jax.nn.sigmoid(rank_s)
        acts_s.append((rank_s * gate).astype(BF16))
        back = slope * (gate * (1.0 + rank_s * (1.0 - gate)))
        tilt = jnp.sum(back.astype(BF16).astype(F32) * rank_s, axis=1, keepdims=True) * (own_scale * own_scale / full_width)
        back_s = back * own_scale
        back_rows = back_s.astype(BF16)
        backs_s.append(back_s)
        tilts.append(tilt)

        @pl.when(sec > 0)
        def _():
            if g == 1:
                back_out[...] = jnp.concatenate(backs_s, axis=1).astype(BF16)
                top = lax.broadcasted_iota(jnp.int32, (8, rows), 0) == 0
                side_out[...] = jnp.where(
                    top, to_row(jnp.concatenate(tilts, axis=0)), to_row(jnp.where(keep, 1.0, 0.0))
                )
                backs.start()
                sides.start()
            for c, cols in enumerate(done_b):
                normed = jnp.dot(back_rows, down[:, cols], preferred_element_type=F32)
                out_b[span, cols] = (
                    kept[span, cols].astype(F32)
                    + gain_ref[:, cols].astype(F32) * normed
                    - sav[span, cols].astype(F32) * tilt
                ).astype(BF16)
                shift(1, out_b, next_gr, g, c).start()

    back_scaled = jnp.concatenate(backs_s, axis=0).astype(BF16)
    act_s = jnp.concatenate(acts_s, axis=0)

    scale_f = scale_of(1)
    if bits:
        for q in range(2):
            finish(form_f, q, bits - 1)
    rank_f = acc_f[...] * scale_f
    act_f = rank_f * jax.nn.sigmoid(rank_f)

    @pl.when(sec < n_sec - 1)
    def _():
        act_out[...] = jnp.concatenate([act_f[:half], act_f[half:]], axis=1).astype(BF16)
        acts.start()

    act_f = act_f.astype(BF16)

    @pl.when(sec < n_sec - 1)
    def _():
        for c, cols in enumerate(done_f):
            grown = jnp.dot(act_f, up[:, cols], preferred_element_type=F32)
            out_f[:, cols] = (fwd[:, cols].astype(F32) + grown).astype(BF16)
            for g in range(2):
                shift(0, out_f, next_in, g, c).start()

    def trade(i, k):
        target = (dp + k) % n_dp
        return pltpu.make_async_remote_copy(
            src_ref=part.at[i, pl.ds(pl.multiple_of(target * share, share), share)],
            dst_ref=part_recv.at[i, k - 1],
            send_sem=dp_send_sem.at[i, k - 1],
            recv_sem=dp_recv_sem.at[i, k - 1],
            device_id={"dp": target},
        )

    for i, (left_side, right_side) in enumerate(((back_scaled, scaled), (act_s, kept))):
        for cols in columns:
            part[i, :, cols] = contract_rows(left_side, right_side[:, cols]).astype(BF16)
        for k in range(1, n_dp):
            trade(i, k).start()

    @pl.when(sec > 0)
    def _():
        raw_ups.wait_recv()
        for k in range(1, n_dp):
            relay(0, k).start()

    @pl.when(sec < n_sec - 1)
    def _():
        raw_downs.wait_recv()
        for k in range(1, n_dp):
            relay(1, k).start()

    for i, out in enumerate((grad_down, grad_up)):
        for k in range(1, n_dp):
            trade(i, k).wait()
        for cols in columns:
            summed = part[i, mine, cols].astype(F32)
            for k in range(1, n_dp):
                summed += part_recv[i, k - 1, :, cols].astype(F32)
            out[:, cols] = (summed * (1.0 / n_dp)).astype(BF16)

    @pl.when(sec == 0)
    def _():
        next_in[...] = jnp.zeros_like(next_in)

    @pl.when(sec == n_sec - 1)
    def _():
        next_gr[...] = jnp.zeros_like(next_gr)

    @pl.when(sec > 0)
    def _():
        for k in range(1, n_dp):
            relay(0, k).wait()
        raw_fwds.wait_recv()
        acts.wait_recv()
        came = act_in[...].astype(F32)
        came = jnp.concatenate([came[:, :rank], came[:, rank:]], axis=0).astype(BF16)
        for a in range(0, raw_f, chunk):
            b = min(a + chunk, raw_f)
            grown = jnp.dot(came, raw_up[:, a:b], preferred_element_type=F32)
            next_in[:, width - raw_f + a:width - raw_f + b] = (raw_fwd[:, a:b].astype(F32) + grown).astype(BF16)

    @pl.when(sec < n_sec - 1)
    def _():
        for k in range(1, n_dp):
            relay(1, k).wait()
        raw_gains.wait_recv()
        raw_savs.wait_recv()
        raw_grads.wait_recv()
        backs.wait_recv()
        sides.wait_recv()
        came = back_in[...].astype(F32)
        far_back = jnp.concatenate([came[:, :rank], came[:, rank:]], axis=0).astype(BF16)
        far_tilt = to_column(side_in[0:1])
        far_keep = to_column(side_in[1:2])
        for a in range(0, raw_b, chunk):
            b = min(a + chunk, raw_b)
            cols = slice(width - raw_b + a, width - raw_b + b)
            normed = jnp.dot(far_back, raw_down[:, a:b], preferred_element_type=F32)
            next_gr[:, cols] = (
                jnp.where(far_keep > 0.5, raw_grad[:, a:b].astype(F32), 0.0)
                + raw_gain[:, cols].astype(F32) * normed
                - raw_sav[:, a:b].astype(F32) * far_tilt
            ).astype(BF16)

    @pl.when(sec < n_sec - 1)
    def _():
        for copy in up_way:
            copy.wait_send()
        for copy in shifts(0):
            copy.wait_send()
        for copy in shifts(1):
            copy.wait_recv()

    @pl.when(sec > 0)
    def _():
        for copy in down_way:
            copy.wait_send()
        for copy in shifts(1):
            copy.wait_send()
        for copy in shifts(0):
            copy.wait_recv()


def place(*refs):
    count = len(refs) // 2
    sems = refs[-1]
    copies = [pltpu.make_async_copy(refs[i], refs[count + i], sems.at[i]) for i in range(count)]
    for copy in copies:
        copy.start()
    for copy in copies:
        copy.wait()


def solution(mesh):
    n_sec, n_ten, n_dp = (mesh.shape[name] for name in ("section", "tensor", "dp"))

    def shards(forward_rows, saved_rows, output_grad, lengths, norm_gain, down_map, up_map):
        rows, width = forward_rows.shape[2:]
        rank = down_map.shape[1]
        share = rank // n_dp
        bits = n_ten.bit_length() - 1
        chunk = min(width, 4 * LANES)
        n_chunk = width // chunk
        raw_f = int(width * RAW_FORWARD) // LANES * LANES
        raw_b = int(width * RAW_BACK) // LANES * LANES
        peers = max(n_ten - 1, 1)
        steps = max(bits, 1)
        vmem = pl.BlockSpec(memory_space=pltpu.VMEM)
        anywhere = pl.BlockSpec(memory_space=pl.ANY)
        flops = 7 * 2 * rows * rank * width
        dma = pltpu.SemaphoreType.DMA
        shapes = ((rows, width),) * 2 + ((share, width),) * 2
        results = pl.pallas_call(
            functools.partial(tick, (n_sec, n_ten, n_dp, chunk)),
            out_shape=tuple(pltpu.VMEM(shape, BF16) for shape in shapes),
            in_specs=[anywhere, anywhere, anywhere, pl.BlockSpec(memory_space=pltpu.SMEM), vmem, anywhere, anywhere],
            out_specs=(vmem,) * 4,
            scratch_shapes=[
                pltpu.VMEM((rows, width), BF16),
                pltpu.VMEM((rows, width), BF16),
                pltpu.VMEM((rows, width), BF16),
                pltpu.VMEM((rank, width), BF16),
                pltpu.VMEM((rank, width), BF16),
                pltpu.VMEM((rows, width), BF16),
                pltpu.VMEM((rows, rank), F32),
                pltpu.VMEM((rows, 2 * rank), F32),
                pltpu.VMEM((steps, rows, rank), BF16),
                pltpu.VMEM((steps, rows, rank), BF16),
                pltpu.VMEM((steps, rows, 2 * rank), BF16),
                pltpu.VMEM((steps, rows, 2 * rank), BF16),
                pltpu.VMEM((rows, width), BF16),
                pltpu.VMEM((rows, width), BF16),
                pltpu.VMEM((2, rank, width), BF16),
                pltpu.VMEM((2, max(n_dp - 1, 1), share, width), BF16),
                pltpu.VMEM((rows // 2, 2 * rank), BF16),
                pltpu.VMEM((rows // 2, 2 * rank), BF16),
                pltpu.VMEM((rows // 2, 2 * rank), BF16),
                pltpu.VMEM((rows // 2, 2 * rank), BF16),
                pltpu.VMEM((8, rows), F32),
                pltpu.VMEM((8, rows), F32),
                pltpu.VMEM((2, 8, rows), F32),
                pltpu.VMEM((2, peers, 8, rows), F32),
                dma((2, peers)),
                dma((2, peers)),
                pltpu.VMEM((rows, raw_f), BF16),
                pltpu.VMEM((rank, raw_f), BF16),
                pltpu.VMEM((rows, raw_b), BF16),
                pltpu.VMEM((rows, raw_b), BF16),
                pltpu.VMEM((rank, raw_b), BF16),
                pltpu.VMEM((1, width), BF16),
                dma((5,)),
                dma((2, steps)),
                dma((2, steps)),
                dma((BLOCKS, steps)),
                dma((BLOCKS, steps)),
                dma((2, 2, n_chunk)),
                dma((2, 2, n_chunk)),
                dma((2, max(n_dp - 1, 1))),
                dma((2, max(n_dp - 1, 1))),
                dma((9,)),
                dma((9,)),
                dma((2, max(n_dp - 1, 1))),
                dma((2, max(n_dp - 1, 1))),
            ],
            compiler_params=pltpu.CompilerParams(collective_id=0, has_side_effects=True),
            cost_estimate=pl.CostEstimate(
                flops=flops, bytes_accessed=16 * rows * width, transcendentals=4 * rows * rank
            ),
            name="tick",
        )(
            forward_rows[0, 0], saved_rows[0, 0], output_grad[0, 0], lengths[0], norm_gain, down_map[0], up_map[0]
        )
        next_inputs, next_grads, grad_down, grad_up = pl.pallas_call(
            place,
            out_shape=tuple(jax.ShapeDtypeStruct(shape, BF16) for shape in shapes),
            in_specs=[vmem] * 4,
            out_specs=(anywhere,) * 4,
            scratch_shapes=[dma((4,))],
            name="place",
        )(*[pltpu.with_memory_space_constraint(x, pltpu.VMEM) for x in results])
        return next_inputs[None, None], next_grads[None, None], grad_down[None], grad_up[None]

    row_spec = P("section", "dp", None, "tensor")
    map_spec = P("section", None, "tensor")
    part_spec = P("section", "dp", "tensor")
    return jax.shard_map(
        shards,
        mesh=mesh,
        in_specs=(row_spec, row_spec, row_spec, P("section", "dp"), P("section", "tensor"), map_spec, map_spec),
        out_specs=(row_spec, row_spec, part_spec, part_spec),
        check_vma=False,
    )
```
